32 devices in a mesh: dp: 8 (over z, y), mp: 4 (over x, core).
Axes of the slice: x: 2, y: 2, z: 4, core: 2. Of those that a mesh axis runs over, the one named last changes fastest.
Arguments:
- pred_input: bfloat16 [512, 256, 384], P('dp'), may hold values from -6 to 6
- proj_weight: bfloat16 [384, 1280], P('dp', 'mp'), may hold values from -0.3125 to 0.3125
- proj_bias: float32 [1280], P('mp'), may hold values from -3 to 3
- targets: bfloat16 [512, 256, 1280], P('dp', None, 'mp'), may hold values from -6 to 6
- block_masks: int32 [512, 4, 256], P('dp'), may hold values from 0 to 1, as said below
Outputs:
- loss: float32 [], replicated
- clip_scale: float32 [], replicated
- grad_weight: float32 [384, 1280], P('dp', 'mp')
- grad_bias: float32 [1280], P('mp')
The draws below stay inside these ranges and needn't reach their ends.
Inputs may be any that keep to these rules, and one draw needn't show every extreme that they name: `block_masks`: each of an image's 4 target blocks is a nonempty rectangle of patches on the 16 x 16 grid (row-major patch order); blocks may intersect.
All inputs are finite; a program needn't handle non-finite values.
Results may differ from the reference program's by a relative error of at most 0.0003.
Values may be sent and summed in bfloat16 or wider, within the bound.
A program may use at most 192 MiB of HBM per device.

```python
import jax
import jax.numpy as jnp
from jax import lax

D = 1280
E = 384
GRID = 16
BLOCKS = 4
IMG_DEV = 64
PATCHES = 256
IMAGES = 512


def draw_block_masks(key, part):
    keys = jax.random.split(key, 4)
    lowest = max(1, GRID * 5 // 16)
    highest = GRID // 2 + 1
    heights = jax.random.randint(keys[0], (IMAGES, BLOCKS, 1), lowest, highest)
    widths = jax.random.randint(keys[1], (IMAGES, BLOCKS, 1), lowest, highest)
    top_raw = jax.random.randint(keys[2], (IMAGES, BLOCKS, 1), 0, 1 << 20)
    left_raw = jax.random.randint(keys[3], (IMAGES, BLOCKS, 1), 0, 1 << 20)
    top_row = top_raw % (GRID - heights + 1)
    left_col = left_raw % (GRID - widths + 1)
    places = jnp.arange(GRID * GRID, dtype=jnp.int32)
    row_of = (places // GRID)[None, None, :]
    col_of = (places % GRID)[None, None, :]
    inside = (row_of >= top_row) & (row_of < top_row + heights) & (col_of >= left_col) & (col_of < left_col + widths)
    return inside.astype(jnp.int32)


def shard_levels(own_key, dims, pieces, low, high):
    level = 1.0
    for axis_at, blocks in pieces:
        draws = jax.random.uniform(jax.random.fold_in(jax.random.fold_in(own_key, 6), axis_at), (blocks,), jnp.float32, low / len(pieces), high / len(pieces))
        level = level * jnp.repeat(jnp.exp(draws), dims[axis_at] // blocks).reshape((-1,) + (1,) * (len(dims) - 1 - axis_at))
    return level


def scatter_about(rng, shape, spread, bound, pieces=(), held_as=jnp.bfloat16):
    values = spread * jax.random.normal(rng, shape, jnp.float32)
    if pieces:
        values = values * shard_levels(rng, shape, pieces, -0.22, 0.18)
    return jnp.clip(values, -bound, bound).astype(held_as)


def setup_inputs(seed: int = 0) -> dict:
    key_list = jax.random.split(jax.random.key(seed), 6)
    return {
        "pred_input": scatter_about(key_list[0], (IMAGES, PATCHES, E), 1.0, 6.0, ((0, 8),)),
        "proj_weight": scatter_about(key_list[1], (E, D), E ** -0.5, 0.3125, ((0, 8), (1, 4))),
        "proj_bias": scatter_about(key_list[2], (D,), 0.5, 3.0, ((0, 4),), jnp.float32),
        "targets": scatter_about(key_list[3], (IMAGES, PATCHES, D), 1.0, 6.0, ((0, 8), (2, 4))),
        "block_masks": draw_block_masks(jax.random.fold_in(key_list[5], 71), 0),
    }


def reference(pred_input, proj_weight, proj_bias, targets, block_masks):
    groups = IMAGES // IMG_DEV
    inputs_grouped = pred_input.reshape(groups, IMG_DEV * PATCHES, E)
    targets_grouped = targets.reshape(groups, IMG_DEV * PATCHES, D)
    coverage_all = lax.optimization_barrier(jnp.sum(block_masks, axis=1)).astype(jnp.float32)
    coverage_grouped = coverage_all.reshape(groups, IMG_DEV * PATCHES, 1)

    def step(carry, batch):
        grad_acc, bias_acc, loss_acc, count_acc = carry
        inputs_here, targets_here, coverage = batch
        target_f = targets_here.astype(jnp.float32)
        mean_feat = lax.optimization_barrier(jnp.mean(target_f, axis=1, keepdims=True))
        centered = target_f - mean_feat
        variance = lax.optimization_barrier(jnp.mean(centered * centered, axis=1, keepdims=True))
        tnorm = centered / jnp.sqrt(variance + 1e-05)
        pred = jnp.dot(inputs_here, proj_weight, preferred_element_type=jnp.float32) + proj_bias
        differ = pred - tnorm
        magnitude = jnp.abs(differ)
        smooth = jnp.where(magnitude < 1.0, 0.5 * differ * differ, magnitude - 0.5)
        clipped = coverage * jnp.clip(differ, -1.0, 1.0)
        source = clipped.astype(jnp.bfloat16)
        grad_acc = grad_acc + lax.dot_general(inputs_here, source, (((0,), (0,)), ((), ())), preferred_element_type=jnp.float32)
        bias_acc = bias_acc + lax.optimization_barrier(jnp.sum(clipped, axis=0))
        loss_acc = loss_acc + jnp.sum(coverage * smooth)
        count_acc = count_acc + jnp.sum(coverage)
        return ((grad_acc, bias_acc, loss_acc, count_acc), None)
    start = (jnp.zeros((E, D), jnp.float32), jnp.zeros((D,), jnp.float32), jnp.zeros((), jnp.float32), jnp.zeros((), jnp.float32))
    (grad_acc, bias_acc, loss_acc, total), unused = lax.scan(step, start, (inputs_grouped, targets_grouped, coverage_grouped))
    grad_w = grad_acc / total
    grad_b = bias_acc / total
    norm = jnp.sqrt(jnp.sum(grad_w * grad_w) + jnp.sum(grad_b * grad_b))
    clip_scale = jnp.minimum(1.0, 1.0 / (norm + 1e-06))
    loss = loss_acc / total / D
    return (loss, clip_scale, clip_scale * grad_w, clip_scale * grad_b)
```

```python
import functools

import jax
import jax.numpy as jnp
from jax import lax
from jax.experimental import pallas as pl
from jax.experimental.pallas import tpu as pltpu
from jax.sharding import PartitionSpec as P

F32 = jnp.float32
BF16 = jnp.bfloat16
MESH = pl.DeviceIdType.MESH
LANES = 128
GROUP = 8
PAIR = 2
CHUNK = 16
TILE = 256
ROWS = 32
SWEEP = 16


def pad_to(n, m):
    return (n + m - 1) // m * m


def layout(rows):
    half = pad_to(rows, 8)
    sums = half + pad_to(rows // 2, 8)
    late = sums + 8
    return half, sums, late, late + pad_to(rows, 8)


def finish(ndp, nmp, sum_ref, fin_ref, loss_ref, clip_ref, gw_ref, gb_ref):
    rows, feat = gw_ref.shape
    half_at, sums_at, late_at, _ = layout(rows)
    tiles = pad_to(feat, LANES) // LANES
    count = sum_ref[sums_at + tiles + 1:sums_at + tiles + 2, 0:1]
    square, loss = fin_ref[:, 0:1], fin_ref[:, 1:2]
    norm = jnp.sqrt(square) / count
    scale = jnp.minimum(1.0, 1.0 / (norm + 1e-06))
    factor = scale / count
    loss_ref[...] = loss / count * (1.0 / (feat * nmp * ndp))
    clip_ref[...] = scale
    gw_ref[:, :LANES] = sum_ref[late_at:late_at + rows, :] * factor
    gw_ref[:, LANES:2 * LANES] = sum_ref[:rows, :] * factor
    half = LANES // 2
    packed = sum_ref[half_at:half_at + rows // 2, :] * factor
    gw_ref[:rows // 2, 2 * LANES:] = packed[:, :half]
    gw_ref[rows // 2:, 2 * LANES:] = packed[:, half:]
    for n in range(tiles):
        stop = min((n + 1) * LANES, feat)
        bias = sum_ref[sums_at + n:sums_at + n + 1, :] * factor
        gb_ref[n * LANES:stop] = bias[0, :stop - n * LANES]


def kernel(ndp, nmp, x_hbm, w_ref, b_ref, t_hbm, m_hbm,
           out_ref, fin_ref,
           xv, tv, mv, wall, wfull, wt, ones, bcol, brow, ssend, srecv, rbuf, mbuf, cbuf,
           pa, pb, sa, sb, s2, acc1, acc2, gacc, lacc,
           gs1, pv1, gm1, gr1, gs2, pv2, gm2, gr2, fsend, frecv,
           xsem, tsem, msem, wss, wrs, sss, srs, ps1, pr1, g1s, g1r, ps2, pr2, g2s, g2r, fss, frs):
    images, halves, feat, _ = tv.shape
    patches = halves * LANES
    parts, _, _ = xv.shape
    width = parts * LANES
    rows = w_ref.shape[0]
    early = s2.shape[2]
    rest = feat - early
    pieces = feat // ROWS
    dp, mp = lax.axis_index("dp"), lax.axis_index("mp")
    inner_dp, outer_dp = gs1.shape[0], gs1.shape[1]
    near, far = lax.rem(dp, inner_dp), dp // inner_dp
    featp = bcol.shape[0]
    groups = images // GROUP
    steps = images // PAIR
    ntot = ndp * nmp
    me = dp * nmp + mp
    feat_full = feat * nmp
    mxus = range(2)

    def scoped(*accs):
        proj = [list(accs[q * pieces:(q + 1) * pieces]) for q in mxus]
        grad_acc = list(accs[2 * pieces:2 * pieces + 2])
        late_acc = list(accs[2 * pieces + 2:2 * pieces + 4])

        def t_copy(g, h):
            s = pl.ds(g * GROUP, GROUP)
            return pltpu.make_async_copy(t_hbm.at[s, :, pl.ds(h * LANES, LANES)], tv.at[s, h], tsem.at[h, g])

        def x_copy(g, j):
            s = pl.ds(g * GROUP * patches, GROUP * patches)
            return pltpu.make_async_copy(x_hbm.at[s, pl.ds(j * LANES, LANES)], xv.at[j, s], xsem.at[j, g])

        def x_start(g):
            for j in range(parts):
                x_copy(g, j).start()

        def x_wait(g):
            for j in range(parts):
                x_copy(g, j).wait()

        m_copy = pltpu.make_async_copy(m_hbm, mv, msem)
        barrier = pltpu.get_barrier_semaphore()

        def greet(o, _):
            d = lax.rem(me + o, ntot)
            pl.semaphore_signal(barrier, inc=1, device_id=(d // nmp, lax.rem(d, nmp)), device_id_type=MESH)
            return 0

        lax.fori_loop(1, ntot, greet, 0)
        m_copy.start()
        for g in range(groups):
            for h in range(halves):
                t_copy(g, h).start()

        gacc[...] = jnp.zeros_like(gacc)
        lacc[...] = jnp.zeros_like(lacc)
        sb[...] = jnp.zeros_like(sb)
        acc1[...] = jnp.zeros_like(acc1)
        wfull[...] = jnp.zeros_like(wfull)
        brow[...] = jnp.zeros_like(brow)
        if rows % 16:
            gs1[...] = jnp.zeros_like(gs1)
            gs2[...] = jnp.zeros_like(gs2)
        lane = lax.broadcasted_iota(jnp.int32, ones.shape, 1)
        ones[...] = jnp.where(lane < 3, 1.0, 0.0).astype(BF16)
        brow[0:1, :feat] = b_ref[...].reshape(1, feat)
        bcol[...] = jnp.transpose(jnp.broadcast_to(brow[0:1, :], (LANES, featp)))
        bias = bcol[:feat, :]
        high = bias.astype(BF16)
        left = bias - high.astype(F32)
        mid = left.astype(BF16)
        low = (left - mid.astype(F32)).astype(BF16)
        lane = lax.broadcasted_iota(jnp.int32, (feat, LANES), 1)
        pick = jnp.where(lane == 0, high.astype(F32), jnp.where(lane == 1, mid.astype(F32), low.astype(F32)))
        wt[:, width:] = jnp.where(lane < 3, pick, 0.0).astype(BF16)
        for q in mxus:
            blank = jnp.zeros((ROWS, TILE), BF16)
            pltpu.matmul_acc_lhs(proj[q][0], blank, load_staged_rhs=0)
            pltpu.matmul_acc_lhs(proj[q][0], blank, load_staged_rhs=1)
            for ref in proj[q] + [grad_acc[q], late_acc[q]]:
                pltpu.matmul_pop(ref)

        pl.semaphore_wait(barrier, ntot - 1)

        def w_copy(o):
            return pltpu.make_async_remote_copy(
                src_ref=w_ref, dst_ref=wall.at[o - 1], send_sem=wss.at[o - 1], recv_sem=wrs.at[o - 1],
                device_id=(lax.rem(dp + o, ndp), mp), device_id_type=MESH)

        for o in range(1, ndp):
            w_copy(o).start()

        def s_copy(o, g):
            return pltpu.make_async_remote_copy(
                src_ref=ssend.at[g], dst_ref=srecv.at[o - 1, g],
                send_sem=sss.at[o - 1, g], recv_sem=srs.at[o - 1, g],
                device_id=(dp, lax.rem(mp + o, nmp)), device_id_type=MESH)

        m_copy.wait()

        def cover(g, _):
            block = [jnp.sum(mv[g * GROUP + j], axis=0, keepdims=True) for j in range(GROUP)]
            cbuf[pl.ds(pl.multiple_of(g * GROUP, GROUP), GROUP), :] = jnp.concatenate(block, axis=0).astype(F32)
            return 0

        lax.fori_loop(0, groups, cover, 0)

        def stats(g, _):
            for h in range(halves):
                t_copy(g, h).wait()

            @pl.when(g >= 2)
            def _():
                x_start(g - 2)

            sums, squares = [], []
            for j in range(GROUP):
                i = g * GROUP + j
                for h in range(halves):
                    part = jnp.zeros((CHUNK, LANES), F32)
                    for c in range(0, feat, CHUNK):
                        part = part + tv[i, h, c:c + CHUNK, :].astype(F32)
                    total = jnp.sum(part, axis=0, keepdims=True)
                    mean = total * (1.0 / feat)
                    part = jnp.zeros((CHUNK, LANES), F32)
                    for c in range(0, feat, CHUNK):
                        centred = tv[i, h, c:c + CHUNK, :].astype(F32) - mean
                        part = part + centred * centred
                    sums.append(total)
                    squares.append(jnp.sum(part, axis=0, keepdims=True))
            for h in range(halves):
                block = jnp.concatenate(sums[h::halves] + squares[h::halves], axis=0)
                ssend[g, :, h * LANES:(h + 1) * LANES] = block

            @pl.when(g > 0)
            def _():
                for o in range(1, nmp):
                    s_copy(o, g - 1).start()

            return 0

        lax.fori_loop(0, groups, stats, 0)
        for g in range(groups - 2, groups):
            x_start(g)

        for o in range(1, ndp):
            w_copy(o).wait_recv()
        for o in range(1, nmp):
            s_copy(o, groups - 1).start()
        for k in range(ndp):
            slot = lax.rem(dp - k + ndp, ndp)
            other = wall[jnp.maximum(slot - 1, 0)].astype(F32)
            block = jnp.where(slot == 0, w_ref[...].astype(F32), other)
            wfull[k * rows:(k + 1) * rows, :feat] = block
        wt[:, :width] = jnp.transpose(wfull[...])[:feat].astype(BF16)

        def x_tile(img, part):
            at = pl.ds(pl.multiple_of(img * patches, patches), patches)
            left = xv[2 * part, at, :]
            right = xv[2 * part + 1, at, :] if 2 * part + 1 < parts else ones[...]
            return jnp.concatenate([left, right], axis=1)

        def push_project(k, part):
            for q in mxus:
                tile = x_tile(PAIR * k + q, part)
                pltpu.matmul_push_rhs(tile, staging_register=part, mxu_index=q, transpose=True)

        def project(part, c):
            lhs = wt[c * ROWS:(c + 1) * ROWS, part * TILE:(part + 1) * TILE]
            for q in mxus:
                pltpu.matmul_acc_lhs(proj[q][c], lhs, load_staged_rhs=part if c == 0 else None)

        def push_gradient(k, g):
            for q in mxus:
                pltpu.matmul_push_rhs(x_tile(PAIR * k + g, q), staging_register=g, mxu_index=q)

        def gradient(s_ref, g):
            lhs = s_ref[:, g * patches:(g + 1) * patches]
            for q in mxus:
                pltpu.matmul_acc_lhs(grad_acc[q], lhs, load_staged_rhs=g)

        def keep(p_ref, c):
            for q in mxus:
                p_ref[q, c * ROWS:(c + 1) * ROWS, :] = pltpu.matmul_pop(proj[q][c])

        def pointwise(p_ref, s_ref, k, c, stat, loss):
            for f in range(c * ROWS, (c + 1) * ROWS, CHUNK):
                total = jnp.zeros((CHUNK, LANES), F32)
                for g in range(PAIR):
                    for h in range(halves):
                        lanes = slice(h * LANES, (h + 1) * LANES)
                        r, m, cov = [v[:, lanes] for v in stat[g]]
                        t = tv[PAIR * k + g, h, f:f + CHUNK, :].astype(F32)
                        differ = p_ref[g, f:f + CHUNK, lanes] + (m - t * r)
                        clipped = jnp.clip(differ, -1.0, 1.0)
                        source = clipped * cov
                        loss[h] = loss[h] + source * (differ - 0.5 * clipped)
                        total = total + source
                        if f < early:
                            s2[PAIR * k + g, h, f:f + CHUNK, :] = source.astype(BF16)
                        else:
                            at = g * patches + h * LANES
                            s_ref[f - early:f - early + CHUNK, at:at + LANES] = source.astype(BF16)
                gacc[f:f + CHUNK, :] += total

        def step(k, p_in, p_out, s_out, s_in):
            last = steps - 1
            back, ahead, beyond = jnp.maximum(k - 1, 0), jnp.minimum(k + 1, last), jnp.minimum(k + 2, last)
            stat = [[v[pl.ds(PAIR * k + g, 1), :] for v in (rbuf, mbuf, cbuf)] for g in range(PAIR)]
            loss = [jnp.zeros((CHUNK, LANES), F32)] * halves
            todo = [functools.partial(project, 0, c) for c in range(pieces)]
            todo.append(functools.partial(push_project, ahead, 1))
            todo += [functools.partial(project, 1, c) for c in range(pieces)]
            todo.append(functools.partial(push_gradient, back, 0))
            todo.append(functools.partial(gradient, s_in, 0))
            todo.append(functools.partial(push_gradient, back, 1))
            todo.append(functools.partial(push_project, beyond, 0))
            todo.append(functools.partial(gradient, s_in, 1))
            done = 0
            for c in range(pieces):
                upto = min(len(todo), pl.cdiv(len(todo) * (c + 1), pieces))
                for op in todo[done:upto]:
                    op()
                done = upto
                pointwise(p_in, s_out, k, c, stat, loss)
            for c in range(pieces):
                keep(p_out, c)
            lacc[...] += functools.reduce(jnp.add, loss)

        x_wait(0)
        push_project(0, 0)
        for c in range(pieces):
            project(0, c)
        push_project(0, 1)
        for c in range(pieces):
            project(1, c)
        push_project(1, 0)
        for c in range(pieces):
            keep(pa, c)
        per_group = GROUP // PAIR

        def outer(g, _):
            @pl.when(g + 1 < groups)
            def _():
                x_wait(g + 1)

            for o in range(1, nmp):
                s_copy(o, g).wait_recv()
            parts_in = [ssend[g]] + [srecv[o - 1, g] for o in range(1, nmp)]
            sums = [p[:GROUP] for p in parts_in]
            mean = functools.reduce(jnp.add, sums) * (1.0 / feat_full)
            var = functools.reduce(jnp.add, [p[GROUP:] for p in parts_in])
            for s in sums:
                gap = s * (1.0 / feat) - mean
                var = var + feat * (gap * gap)
            rstd = lax.rsqrt(var * (1.0 / feat_full) + 1e-05)
            here = pl.ds(pl.multiple_of(g * GROUP, GROUP), GROUP)
            rbuf[here, :] = rstd
            mbuf[here, :] = mean * rstd

            def inner(j, _):
                k = g * per_group + 2 * j
                step(k, pa, pb, sa, sb)
                pl.delay(1)
                step(k + 1, pb, pa, sb, sa)
                return 0

            lax.fori_loop(0, per_group // 2, inner, 0)
            return 0

        lax.fori_loop(0, groups, outer, 0)
        project(0, 0)
        for q in mxus:
            pltpu.matmul_pop(proj[q][0])
        for g in range(PAIR):
            push_gradient(steps - 1, g)
            gradient(sb, g)
        acc1[:rest, :TILE] = pltpu.matmul_pop(grad_acc[0])
        acc1[:rest, TILE:] = pltpu.matmul_pop(grad_acc[1])[:, :width - TILE]

        half_at, sums_at, late_at, total_rows = layout(rows)
        tiles = featp // LANES
        bias_part = jnp.sum(jnp.transpose(gacc[...]), axis=0, keepdims=True)
        loss_part = jnp.sum(lacc[...], keepdims=True)
        count_part = jnp.sum(cbuf[...], keepdims=True)
        at_row = lax.broadcasted_iota(jnp.int32, (8, LANES), 0)
        extra = jnp.where(at_row == tiles, loss_part, count_part)
        for n in range(tiles):
            extra = jnp.where(at_row == n, bias_part[:, n * LANES:(n + 1) * LANES], extra)
        full = jnp.transpose(acc1[...])
        half = LANES // 2
        for k in range(ndp):
            slot = gs1.at[k % inner_dp, k // inner_dp]
            mine = full[k * rows:(k + 1) * rows]
            slot[:rows, :] = mine[:, :LANES]
            slot[half_at:half_at + rows // 2, :] = jnp.concatenate(
                [mine[:rows // 2, LANES:LANES + half], mine[rows // 2:, LANES:LANES + half]], axis=1)
            slot[sums_at:, :] = extra

        other = 1 - near

        def p_copy(o, bufs):
            src, dst, _, _, ss, rs, _, _ = bufs
            to = lax.rem(far + o, outer_dp)
            return pltpu.make_async_remote_copy(
                src_ref=src.at[other, to], dst_ref=dst.at[o], send_sem=ss.at[o], recv_sem=rs.at[o],
                device_id=(far * inner_dp + other, mp), device_id_type=MESH)

        def g_copy(o, bufs):
            _, _, src, dst, _, _, ss, rs = bufs
            to = lax.rem(far + o, outer_dp)
            return pltpu.make_async_remote_copy(
                src_ref=src.at[o - 1], dst_ref=dst.at[o - 1], send_sem=ss.at[o - 1], recv_sem=rs.at[o - 1],
                device_id=(to * inner_dp + near, mp), device_id_type=MESH)

        first = (gs1, pv1, gm1, gr1, ps1, pr1, g1s, g1r)
        second = (gs2, pv2, gm2, gr2, ps2, pr2, g2s, g2r)
        order = list(range(1, outer_dp)) + [0]
        for o in order:
            p_copy(o, first).start()

        def push_late(img, r):
            for q in mxus:
                pltpu.matmul_push_rhs(x_tile(img, q), staging_register=r, mxu_index=q)

        push_late(0, 0)

        def sweep(k, _):
            for g in range(SWEEP):
                img = k * SWEEP + g
                push_late(jnp.minimum(img + 1, images - 1), (g + 1) % 2)
                lhs = jnp.concatenate([s2[img, h, :, :] for h in range(halves)], axis=1)
                for q in mxus:
                    pltpu.matmul_acc_lhs(late_acc[q], lhs, load_staged_rhs=g % 2)
            return 0

        lax.fori_loop(0, images // SWEEP, sweep, 0)
        acc2[:, :TILE] = pltpu.matmul_pop(late_acc[0])
        acc2[:, TILE:] = pltpu.matmul_pop(late_acc[1])[:, :width - TILE]
        for q in mxus:
            pltpu.matmul_acc_lhs(late_acc[q], jnp.zeros((early, TILE), BF16), load_staged_rhs=0)
            pltpu.matmul_pop(late_acc[q])
        full = jnp.transpose(acc2[...])
        for k in range(ndp):
            gs2[k % inner_dp, k // inner_dp, :rows, :] = full[k * rows:(k + 1) * rows]
        for o in order:
            p_copy(o, second).start()

        pairs = []
        for bufs in (first, second):
            src, dst, mid_buf = bufs[:3]
            for o in order:
                p_copy(o, bufs).wait_recv()
                pair = src[near, lax.rem(far + o, outer_dp)] + dst[o]
                if o:
                    mid_buf[o - 1] = pair
                    g_copy(o, bufs).start()
            pairs.append(pair)
        for n, bufs in enumerate((first, second)):
            for o in range(1, outer_dp):
                g_copy(o, bufs).wait_recv()
                pairs[n] = pairs[n] + bufs[3][o - 1]
        out_ref[:late_at, :] = pairs[0]
        out_ref[late_at:, :] = pairs[1]
        head = pairs[0][:sums_at]
        sums = pairs[0][sums_at:]
        bias_grad = sums[:tiles]
        square = jnp.sum(head * head, keepdims=True) + jnp.sum(pairs[1] * pairs[1], keepdims=True)
        bias_square = jnp.sum(bias_grad * bias_grad, keepdims=True)
        lane = lax.broadcasted_iota(jnp.int32, (1, LANES), 1)
        fsend[...] = jnp.where(lane == 0, square + bias_square * (1.0 / ndp), sums[tiles:tiles + 1, :])

        def f_copy(o):
            d = lax.rem(me + o, ntot)
            return pltpu.make_async_remote_copy(
                src_ref=fsend, dst_ref=frecv.at[o - 1], send_sem=fss.at[o - 1], recv_sem=frs.at[o - 1],
                device_id=(d // nmp, lax.rem(d, nmp)), device_id_type=MESH)

        def f_start(o, _):
            f_copy(o).start()
            return 0

        def f_wait(o, _):
            f_copy(o).wait_recv()
            return 0

        lax.fori_loop(1, ntot, f_start, 0)

        for o in range(1, ndp):
            w_copy(o).wait_send()
        for bufs in (first, second):
            for o in order:
                p_copy(o, bufs).wait_send()
                if o:
                    g_copy(o, bufs).wait_send()

        def s_drain(g, _):
            for o in range(1, nmp):
                s_copy(o, g).wait_send()
            return 0

        def f_drain(o, _):
            f_copy(o).wait_send()
            return 0

        lax.fori_loop(0, groups, s_drain, 0)
        lax.fori_loop(1, ntot, f_wait, 0)
        fin_ref[...] = fsend[...] + jnp.sum(frecv[...], axis=0)
        lax.fori_loop(1, ntot, f_drain, 0)

    tile = [pltpu.ACC(q)((ROWS, TILE), F32) for q in mxus]
    refs = [tile[0]] * pieces + [tile[1]] * pieces
    refs += [pltpu.ACC(q)((rest, TILE), F32) for q in mxus]
    refs += [pltpu.ACC(q)((early, TILE), F32) for q in mxus]
    pl.run_scoped(scoped, *refs)


def body(pred_input, proj_weight, proj_bias, targets, block_masks):
    images, patches, width = pred_input.shape
    feat = targets.shape[2]
    rows = proj_weight.shape[0]
    blocks = block_masks.shape[1]
    ndp, nmp = lax.axis_size("dp"), lax.axis_size("mp")
    ntot = ndp * nmp
    featp = pad_to(feat, LANES)
    groups = images // GROUP
    halves, parts = patches // LANES, width // LANES
    early = LANES
    rest = feat - early
    dma = pltpu.SemaphoreType.DMA
    vmem = pl.BlockSpec(memory_space=pltpu.VMEM)
    hbm = pl.BlockSpec(memory_space=pl.ANY)
    _, _, late_at, total_rows = layout(rows)
    inner_dp = 2
    outer_dp = ndp // inner_dp
    exchange = []
    for n in (late_at, total_rows - late_at):
        exchange += [
            pltpu.VMEM((inner_dp, outer_dp, n, LANES), F32),
            pltpu.VMEM((outer_dp, n, LANES), F32),
            pltpu.VMEM((outer_dp - 1, n, LANES), F32),
            pltpu.VMEM((outer_dp - 1, n, LANES), F32),
        ]
    exchange_sems = [dma((outer_dp,)), dma((outer_dp,)), dma((outer_dp - 1,)), dma((outer_dp - 1,))]
    summed, final = pl.pallas_call(
        functools.partial(kernel, ndp, nmp),
        out_shape=(
            jax.ShapeDtypeStruct((total_rows, LANES), F32),
            jax.ShapeDtypeStruct((1, LANES), F32),
        ),
        in_specs=[hbm, vmem, vmem, hbm, hbm],
        out_specs=(vmem,) * 2,
        scratch_shapes=[
            pltpu.VMEM((parts, images * patches, LANES), BF16),
            pltpu.VMEM((images, halves, feat, LANES), BF16),
            pltpu.VMEM((images, blocks, patches), jnp.int32),
            pltpu.VMEM((ndp - 1, rows, feat), BF16),
            pltpu.VMEM((width, featp), F32),
            pltpu.VMEM((feat, pad_to(width, TILE)), BF16),
            pltpu.VMEM((patches, LANES), BF16),
            pltpu.VMEM((featp, LANES), F32),
            pltpu.VMEM((8, featp), F32),
            pltpu.VMEM((groups, 2 * GROUP, patches), F32),
            pltpu.VMEM((nmp - 1, groups, 2 * GROUP, patches), F32),
            pltpu.VMEM((images, patches), F32),
            pltpu.VMEM((images, patches), F32),
            pltpu.VMEM((images, patches), F32),
            pltpu.VMEM((PAIR, feat, patches), F32),
            pltpu.VMEM((PAIR, feat, patches), F32),
            pltpu.VMEM((rest, PAIR * patches), BF16),
            pltpu.VMEM((rest, PAIR * patches), BF16),
            pltpu.VMEM((images, halves, early, LANES), BF16),
            pltpu.VMEM((pad_to(rest, LANES), width), F32),
            pltpu.VMEM((early, width), F32),
            pltpu.VMEM((featp, LANES), F32),
            pltpu.VMEM((CHUNK, LANES), F32),
        ] + exchange + [
            pltpu.VMEM((1, LANES), F32),
            pltpu.VMEM((ntot - 1, 1, LANES), F32),
            dma((parts, groups)), dma((halves, groups)), dma(()),
            dma((ndp - 1,)), dma((ndp - 1,)),
            dma((nmp - 1, groups)), dma((nmp - 1, groups)),
        ] + exchange_sems * 2 + [
            dma((ntot - 1,)), dma((ntot - 1,)),
        ],
        compiler_params=pltpu.CompilerParams(
            collective_id=0, has_side_effects=True, vmem_limit_bytes=60 * 1024 * 1024
        ),
    )(
        pred_input.reshape(images * patches, width),
        proj_weight,
        proj_bias,
        jnp.swapaxes(targets, 1, 2),
        block_masks,
    )
    loss, clip, gw, gb = pl.pallas_call(
        functools.partial(finish, ndp, nmp),
        out_shape=(
            jax.ShapeDtypeStruct((1, 1), F32),
            jax.ShapeDtypeStruct((1, 1), F32),
            jax.ShapeDtypeStruct((rows, feat), F32),
            jax.ShapeDtypeStruct((feat,), F32),
        ),
        in_specs=[vmem] * 2,
        out_specs=(vmem,) * 4,
    )(summed, final)
    return loss.reshape(()), clip.reshape(()), gw, gb


def solution(mesh):
    in_specs = (
        P("dp", None, None),
        P("dp", "mp"),
        P("mp"),
        P("dp", None, "mp"),
        P("dp", None, None),
    )
    out_specs = (P(), P(), P("dp", "mp"), P("mp"))
    return jax.shard_map(body, mesh=mesh, in_specs=in_specs, out_specs=out_specs, check_vma=False)
```

```python
import functools

import jax
import jax.numpy as jnp
from jax import lax
from jax.experimental import pallas as pl
from jax.experimental.pallas import tpu as pltpu
from jax.sharding import PartitionSpec as P

F32 = jnp.float32
BF16 = jnp.bfloat16
MESH = pl.DeviceIdType.MESH
LANES = 128
GROUP = 8
PAIR = 2
CHUNK = 16
TILE = 256
ROWS = 32
SWEEP = 16
HAND = 5


def pad_to(n, m):
    return (n + m - 1) // m * m


def layout(rows):
    half = pad_to(rows, 8)
    sums = half + pad_to(rows // 2, 8)
    late = sums + 8
    return half, sums, late, late + pad_to(rows, 8)


def finish(ndp, nmp, sum_ref, loss_ref, clip_ref, gw_ref, gb_ref):
    rows, feat = gw_ref.shape
    half_at, sums_at, late_at, fin_at = layout(rows)
    tiles = pad_to(feat, LANES) // LANES
    count = sum_ref[sums_at + tiles + 1:sums_at + tiles + 2, 0:1]
    square, loss = sum_ref[fin_at:fin_at + 1, 0:1], sum_ref[fin_at:fin_at + 1, 1:2]
    norm = jnp.sqrt(square) / count
    scale = jnp.minimum(1.0, 1.0 / (norm + 1e-06))
    factor = scale / count
    loss_ref[...] = loss / count * (1.0 / (feat * nmp * ndp))
    clip_ref[...] = scale
    gw_ref[:, :LANES] = sum_ref[late_at:late_at + rows, :] * factor
    gw_ref[:, LANES:2 * LANES] = sum_ref[:rows, :] * factor
    half = LANES // 2
    packed = sum_ref[half_at:half_at + rows // 2, :] * factor
    gw_ref[:rows // 2, 2 * LANES:] = packed[:, :half]
    gw_ref[rows // 2:, 2 * LANES:] = packed[:, half:]
    for n in range(tiles):
        stop = min((n + 1) * LANES, feat)
        bias = sum_ref[sums_at + n:sums_at + n + 1, :] * factor
        gb_ref[n * LANES:stop] = bias[0, :stop - n * LANES]


def kernel(ndp, nmp, x_hbm, w_hbm, b_hbm, t_hbm, m_hbm,
           out_hbm,
           xv, tv, mv, w_ref, b_ref, outv, wall, wfull, wt, ones, bcol, brow, ssend, srecv, rbuf, mbuf, cbuf,
           pa, pb, sa, sb, s2, acc1, acc2, gacc, lacc,
           gs1, pv1, gm1, gr1, gs2, pv2, gm2, gr2, fsend, frecv,
           xsem, tsem, msem, bsem, osem, wss, wrs, whs, whr, sss, srs, ps1, pr1, g1s, g1r, ps2, pr2, g2s, g2r, fss, frs):
    images, halves, feat, _ = tv.shape
    patches = halves * LANES
    parts, _, _ = xv.shape
    width = parts * LANES
    rows = w_ref.shape[0]
    early = s2.shape[2]
    rest = feat - early
    pieces = feat // ROWS
    dp, mp = lax.axis_index("dp"), lax.axis_index("mp")
    inner_dp, outer_dp = gs1.shape[0], gs1.shape[1]
    near, far = lax.rem(dp, inner_dp), dp // inner_dp
    featp = bcol.shape[0]
    groups = images // GROUP
    steps = images // PAIR
    ntot = ndp * nmp
    me = dp * nmp + mp
    feat_full = feat * nmp
    mxus = range(2)

    def scoped(*accs):
        proj = [list(accs[q * pieces:(q + 1) * pieces]) for q in mxus]
        grad_acc = list(accs[2 * pieces:2 * pieces + 2])
        late_acc = list(accs[2 * pieces + 2:2 * pieces + 4])

        def t_copy(g, h):
            s = pl.ds(g * GROUP, GROUP)
            return pltpu.make_async_copy(t_hbm.at[s, :, pl.ds(h * LANES, LANES)], tv.at[s, h], tsem.at[g])

        def x_copy(g, j):
            s = pl.ds(g * GROUP * patches, GROUP * patches)
            return pltpu.make_async_copy(x_hbm.at[s, pl.ds(j * LANES, LANES)], xv.at[j, s], xsem.at[g])

        def x_start(g):
            for j in range(parts):
                x_copy(g, j).start()

        def arrive(ref, sem):
            pltpu.make_async_copy(ref, ref, sem).wait()

        def x_wait(g):
            arrive(xv.at[:, pl.ds(g * GROUP * patches, GROUP * patches)], xsem.at[g])

        m_copy = pltpu.make_async_copy(m_hbm, mv, msem.at[0])
        w_own = pltpu.make_async_copy(w_hbm, w_ref, msem.at[1])
        b_own = pltpu.make_async_copy(b_hbm, b_ref, bsem)
        barrier = pltpu.get_barrier_semaphore()

        other = 1 - near

        def line(o):
            return lax.rem(far + o, outer_dp) * inner_dp + near

        partner = far * inner_dp + other
        peers = [(line(o), mp) for o in range(1, outer_dp)] + [(partner, mp)]
        peers += [(dp, lax.rem(mp + o, nmp)) for o in range(1, nmp)]
        for peer in peers:
            pl.semaphore_signal(barrier, inc=1, device_id=peer, device_id_type=MESH)
        w_own.start()
        b_own.start()
        m_copy.start()
        for g in range(groups):
            for h in range(halves):
                t_copy(g, h).start()

        pl.semaphore_wait(barrier, len(peers))

        def w_copy(o):
            return pltpu.make_async_remote_copy(
                src_ref=w_ref, dst_ref=wall.at[dp], send_sem=wss, recv_sem=wrs.at[o],
                device_id=(line(o), mp), device_id_type=MESH)

        def w_hand(o):
            src = lax.rem(far - o + outer_dp, outer_dp) * inner_dp + near
            own = isinstance(o, int) and o == 0
            return pltpu.make_async_remote_copy(
                src_ref=w_ref if own else wall.at[src], dst_ref=wall.at[src], send_sem=whs, recv_sem=whr,
                device_id=(partner, mp), device_id_type=MESH)

        def ranked(offset, n):
            picks = 0
            for f in range(outer_dp):
                near_first = sorted(range(1, outer_dp), key=lambda o: abs((f + offset * o) % outer_dp - f))
                picks = picks + jnp.where(far == f, near_first[n], 0)
            return picks

        w_own.wait()
        for n in reversed(range(outer_dp - 1)):
            w_copy(ranked(1, n)).start()
        w_hand(0).start()

        gacc[...] = jnp.zeros_like(gacc)
        lacc[...] = jnp.zeros_like(lacc)
        sb[...] = jnp.zeros_like(sb)
        acc1[...] = jnp.zeros_like(acc1)
        wfull[...] = jnp.zeros_like(wfull)
        brow[...] = jnp.zeros_like(brow)
        if rows % 16:
            gs1[...] = jnp.zeros_like(gs1)
            gs2[...] = jnp.zeros_like(gs2)
        lane = lax.broadcasted_iota(jnp.int32, ones.shape, 1)
        ones[...] = jnp.where(lane < 3, 1.0, 0.0).astype(BF16)
        b_own.wait()
        brow[0:1, :feat] = b_ref[...].reshape(1, feat)
        bcol[...] = jnp.transpose(jnp.broadcast_to(brow[0:1, :], (LANES, featp)))
        bias = bcol[:feat, :]
        high = bias.astype(BF16)
        left = bias - high.astype(F32)
        mid = left.astype(BF16)
        low = (left - mid.astype(F32)).astype(BF16)
        lane = lax.broadcasted_iota(jnp.int32, (feat, LANES), 1)
        pick = jnp.where(lane == 0, high.astype(F32), jnp.where(lane == 1, mid.astype(F32), low.astype(F32)))
        wt[:, width:] = jnp.where(lane < 3, pick, 0.0).astype(BF16)
        for q in mxus:
            blank = jnp.zeros((ROWS, TILE), BF16)
            pltpu.matmul_acc_lhs(proj[q][0], blank, load_staged_rhs=0)
            pltpu.matmul_acc_lhs(proj[q][0], blank, load_staged_rhs=1)
            for ref in proj[q] + [grad_acc[q], late_acc[q]]:
                pltpu.matmul_pop(ref)

        def s_copy(o, g):
            return pltpu.make_async_remote_copy(
                src_ref=ssend.at[g], dst_ref=srecv.at[o - 1, g],
                send_sem=sss, recv_sem=srs.at[g],
                device_id=(dp, lax.rem(mp + o, nmp)), device_id_type=MESH)

        m_copy.wait()

        def cover(g, _):
            block = [jnp.sum(mv[g * GROUP + j], axis=0, keepdims=True) for j in range(GROUP)]
            cbuf[pl.ds(pl.multiple_of(g * GROUP, GROUP), GROUP), :] = jnp.concatenate(block, axis=0).astype(F32)
            return 0

        lax.fori_loop(0, groups, cover, 0)

        def stats(g, _):
            arrive(tv.at[pl.ds(g * GROUP, GROUP)], tsem.at[g])

            @pl.when(g >= 2)
            def _():
                x_start(g - 2)

            sums, squares = [], []
            for j in range(GROUP):
                i = g * GROUP + j
                for h in range(halves):
                    part = jnp.zeros((CHUNK, LANES), F32)
                    for c in range(0, feat, CHUNK):
                        part = part + tv[i, h, c:c + CHUNK, :].astype(F32)
                    total = jnp.sum(part, axis=0, keepdims=True)
                    mean = total * (1.0 / feat)
                    part = jnp.zeros((CHUNK, LANES), F32)
                    for c in range(0, feat, CHUNK):
                        centred = tv[i, h, c:c + CHUNK, :].astype(F32) - mean
                        part = part + centred * centred
                    sums.append(total)
                    squares.append(jnp.sum(part, axis=0, keepdims=True))
            for h in range(halves):
                block = jnp.concatenate(sums[h::halves] + squares[h::halves], axis=0)
                ssend[g, :, h * LANES:(h + 1) * LANES] = block

            @pl.when(g > 0)
            def _():
                for o in range(1, nmp):
                    s_copy(o, g - 1).start()

            @pl.when(g == HAND)
            def _():
                hand_over(0)

            return 0

        def hand_over(n):
            o = ranked(-1, n)
            w_copy(o).wait_recv()
            w_hand(o).start()

        lax.fori_loop(0, groups, stats, 0)
        for g in range(groups - 2, groups):
            x_start(g)

        for o in range(1, nmp):
            s_copy(o, groups - 1).start()
        for n in range(1, outer_dp - 1):
            hand_over(n)
        wall[dp] = w_ref[...]
        arrive(wall.at[pl.ds(0, outer_dp)], whr)
        for k in range(ndp):
            wfull[k * rows:(k + 1) * rows, :feat] = wall[k].astype(F32)
        wt[:, :width] = jnp.transpose(wfull[...])[:feat].astype(BF16)

        def x_tile(img, part):
            at = pl.ds(pl.multiple_of(img * patches, patches), patches)
            left = xv[2 * part, at, :]
            right = xv[2 * part + 1, at, :] if 2 * part + 1 < parts else ones[...]
            return jnp.concatenate([left, right], axis=1)

        def push_project(k, part):
            for q in mxus:
                tile = x_tile(PAIR * k + q, part)
                pltpu.matmul_push_rhs(tile, staging_register=part, mxu_index=q, transpose=True)

        def project(part, c):
            lhs = wt[c * ROWS:(c + 1) * ROWS, part * TILE:(part + 1) * TILE]
            for q in mxus:
                pltpu.matmul_acc_lhs(proj[q][c], lhs, load_staged_rhs=part if c == 0 else None)

        def push_gradient(k, g):
            for q in mxus:
                pltpu.matmul_push_rhs(x_tile(PAIR * k + g, q), staging_register=g, mxu_index=q)

        def gradient(s_ref, g):
            lhs = s_ref[:, g * patches:(g + 1) * patches]
            for q in mxus:
                pltpu.matmul_acc_lhs(grad_acc[q], lhs, load_staged_rhs=g)

        def keep(p_ref, c):
            for q in mxus:
                p_ref[q, c * ROWS:(c + 1) * ROWS, :] = pltpu.matmul_pop(proj[q][c])

        def pointwise(p_ref, s_ref, k, c, stat, loss):
            for f in range(c * ROWS, (c + 1) * ROWS, CHUNK):
                total = jnp.zeros((CHUNK, LANES), F32)
                for g in range(PAIR):
                    for h in range(halves):
                        lanes = slice(h * LANES, (h + 1) * LANES)
                        r, m, cov = [v[:, lanes] for v in stat[g]]
                        t = tv[PAIR * k + g, h, f:f + CHUNK, :].astype(F32)
                        differ = p_ref[g, f:f + CHUNK, lanes] + (m - t * r)
                        clipped = jnp.clip(differ, -1.0, 1.0)
                        source = clipped * cov
                        loss[h] = loss[h] + source * (differ - 0.5 * clipped)
                        total = total + source
                        if f < early:
                            s2[PAIR * k + g, h, f:f + CHUNK, :] = source.astype(BF16)
                        else:
                            at = g * patches + h * LANES
                            s_ref[f - early:f - early + CHUNK, at:at + LANES] = source.astype(BF16)
                gacc[f:f + CHUNK, :] += total

        def step(k, p_in, p_out, s_out, s_in):
            last = steps - 1
            back, ahead, beyond = jnp.maximum(k - 1, 0), jnp.minimum(k + 1, last), jnp.minimum(k + 2, last)
            stat = [[v[pl.ds(PAIR * k + g, 1), :] for v in (rbuf, mbuf, cbuf)] for g in range(PAIR)]
            loss = [jnp.zeros((CHUNK, LANES), F32)] * halves
            todo = [functools.partial(project, 0, c) for c in range(pieces)]
            todo.append(functools.partial(push_project, ahead, 1))
            todo += [functools.partial(project, 1, c) for c in range(pieces)]
            todo.append(functools.partial(push_gradient, back, 0))
            todo.append(functools.partial(gradient, s_in, 0))
            todo.append(functools.partial(push_gradient, back, 1))
            todo.append(functools.partial(push_project, beyond, 0))
            todo.append(functools.partial(gradient, s_in, 1))
            done = 0
            for c in range(pieces):
                upto = min(len(todo), pl.cdiv(len(todo) * (c + 1), pieces))
                for op in todo[done:upto]:
                    op()
                done = upto
                pointwise(p_in, s_out, k, c, stat, loss)
            for c in range(pieces):
                keep(p_out, c)
            lacc[...] += functools.reduce(jnp.add, loss)

        x_wait(0)
        push_project(0, 0)
        for c in range(pieces):
            project(0, c)
        push_project(0, 1)
        for c in range(pieces):
            project(1, c)
        push_project(1, 0)
        for c in range(pieces):
            keep(pa, c)
        per_group = GROUP // PAIR

        def outer(g, _):
            @pl.when(g + 1 < groups)
            def _():
                x_wait(g + 1)

            arrive(srecv.at[:, g], srs.at[g])
            parts_in = [ssend[g]] + [srecv[o - 1, g] for o in range(1, nmp)]
            sums = [p[:GROUP] for p in parts_in]
            mean = functools.reduce(jnp.add, sums) * (1.0 / feat_full)
            var = functools.reduce(jnp.add, [p[GROUP:] for p in parts_in])
            for s in sums:
                gap = s * (1.0 / feat) - mean
                var = var + feat * (gap * gap)
            rstd = lax.rsqrt(var * (1.0 / feat_full) + 1e-05)
            here = pl.ds(pl.multiple_of(g * GROUP, GROUP), GROUP)
            rbuf[here, :] = rstd
            mbuf[here, :] = mean * rstd

            def inner(j, _):
                k = g * per_group + 2 * j
                step(k, pa, pb, sa, sb)
                pl.delay(1)
                step(k + 1, pb, pa, sb, sa)
                return 0

            lax.fori_loop(0, per_group // 2, inner, 0)
            return 0

        lax.fori_loop(0, groups, outer, 0)
        project(0, 0)
        for q in mxus:
            pltpu.matmul_pop(proj[q][0])
        for g in range(PAIR):
            push_gradient(steps - 1, g)
            gradient(sb, g)
        acc1[:rest, :TILE] = pltpu.matmul_pop(grad_acc[0])
        acc1[:rest, TILE:] = pltpu.matmul_pop(grad_acc[1])[:, :width - TILE]

        half_at, sums_at, late_at, total_rows = layout(rows)
        tiles = featp // LANES
        bias_part = jnp.sum(jnp.transpose(gacc[...]), axis=0, keepdims=True)
        loss_part = jnp.sum(lacc[...], keepdims=True)
        count_part = jnp.sum(cbuf[...], keepdims=True)
        at_row = lax.broadcasted_iota(jnp.int32, (8, LANES), 0)
        extra = jnp.where(at_row == tiles, loss_part, count_part)
        for n in range(tiles):
            extra = jnp.where(at_row == n, bias_part[:, n * LANES:(n + 1) * LANES], extra)
        full = jnp.transpose(acc1[...])
        half = LANES // 2
        for k in range(ndp):
            slot = gs1.at[k % inner_dp, k // inner_dp]
            mine = full[k * rows:(k + 1) * rows]
            slot[:rows, :] = mine[:, :LANES]
            slot[half_at:half_at + rows // 2, :] = jnp.concatenate(
                [mine[:rows // 2, LANES:LANES + half], mine[rows // 2:, LANES:LANES + half]], axis=1)
            slot[sums_at:, :] = extra

        def p_copy(o, bufs):
            src, dst, _, _, ss, rs, _, _ = bufs
            to = lax.rem(far + o, outer_dp)
            return pltpu.make_async_remote_copy(
                src_ref=src.at[other, to], dst_ref=dst.at[o], send_sem=ss, recv_sem=rs.at[o],
                device_id=(partner, mp), device_id_type=MESH)

        def g_copy(o, bufs):
            _, _, src, dst, _, _, ss, rs = bufs
            return pltpu.make_async_remote_copy(
                src_ref=src.at[o - 1], dst_ref=dst.at[o - 1], send_sem=ss, recv_sem=rs,
                device_id=(line(o), mp), device_id_type=MESH)

        first = (gs1, pv1, gm1, gr1, ps1, pr1, g1s, g1r)
        second = (gs2, pv2, gm2, gr2, ps2, pr2, g2s, g2r)
        order = list(range(1, outer_dp)) + [0]
        for o in order:
            p_copy(o, first).start()

        def push_late(img, r):
            for q in mxus:
                pltpu.matmul_push_rhs(x_tile(img, q), staging_register=r, mxu_index=q)

        push_late(0, 0)

        def sweep(k, _):
            for g in range(SWEEP):
                img = k * SWEEP + g
                push_late(jnp.minimum(img + 1, images - 1), (g + 1) % 2)
                lhs = jnp.concatenate([s2[img, h, :, :] for h in range(halves)], axis=1)
                for q in mxus:
                    pltpu.matmul_acc_lhs(late_acc[q], lhs, load_staged_rhs=g % 2)
            return 0

        lax.fori_loop(0, images // SWEEP, sweep, 0)
        acc2[:, :TILE] = pltpu.matmul_pop(late_acc[0])
        acc2[:, TILE:] = pltpu.matmul_pop(late_acc[1])[:, :width - TILE]
        for q in mxus:
            pltpu.matmul_acc_lhs(late_acc[q], jnp.zeros((early, TILE), BF16), load_staged_rhs=0)
            pltpu.matmul_pop(late_acc[q])
        full = jnp.transpose(acc2[...])
        for k in range(ndp):
            gs2[k % inner_dp, k // inner_dp, :rows, :] = full[k * rows:(k + 1) * rows]
        for o in order:
            p_copy(o, second).start()

        pairs = []
        for bufs in (first, second):
            src, dst, mid_buf = bufs[:3]
            for o in order:
                p_copy(o, bufs).wait_recv()
                pair = src[near, lax.rem(far + o, outer_dp)] + dst[o]
                if o:
                    mid_buf[o - 1] = pair
                    g_copy(o, bufs).start()
            pairs.append(pair)
        for n, bufs in enumerate((first, second)):
            arrive(bufs[3], bufs[7])
            for o in range(1, outer_dp):
                pairs[n] = pairs[n] + bufs[3][o - 1]
        outv[:late_at, :] = pairs[0]
        outv[late_at:total_rows, :] = pairs[1]
        head = pairs[0][:sums_at]
        sums = pairs[0][sums_at:]
        bias_grad = sums[:tiles]
        square = jnp.sum(head * head, keepdims=True) + jnp.sum(pairs[1] * pairs[1], keepdims=True)
        bias_square = jnp.sum(bias_grad * bias_grad, keepdims=True)
        lane = lax.broadcasted_iota(jnp.int32, (1, LANES), 1)
        fsend[...] = jnp.where(lane == 0, square + bias_square * (1.0 / ndp), sums[tiles:tiles + 1, :])

        def f_copy(d):
            return pltpu.make_async_remote_copy(
                src_ref=fsend, dst_ref=frecv.at[me], send_sem=fss, recv_sem=frs,
                device_id=(d // nmp, lax.rem(d, nmp)), device_id_type=MESH)

        def f_start(o, _):
            f_copy(o + jnp.where(o >= me, 1, 0)).start()
            return 0

        lax.fori_loop(0, ntot - 1, f_start, 0)
        frecv[me] = fsend[...]
        body_out = pltpu.make_async_copy(outv.at[pl.ds(0, total_rows)], out_hbm.at[pl.ds(0, total_rows)], osem.at[0])
        body_out.start()
        tail_out = pltpu.make_async_copy(outv.at[pl.ds(total_rows, 8)], out_hbm.at[pl.ds(total_rows, 8)], osem.at[1])

        arrive(wall.at[pl.ds(0, outer_dp - 1)], wss)
        arrive(wall.at[pl.ds(0, outer_dp)], whs)
        for bufs in (first, second):
            arrive(bufs[0].at[0], bufs[4])
            arrive(bufs[2], bufs[6])
        arrive(srecv, sss)
        body_out.wait()
        everyone = frecv.at[pl.ds(0, ntot - 1)]
        arrive(everyone, frs)
        outv[total_rows:, :] = jnp.broadcast_to(jnp.sum(frecv[...], axis=0), (8, LANES))
        tail_out.start()
        arrive(everyone, fss)
        tail_out.wait()

    tile = [pltpu.ACC(q)((ROWS, TILE), F32) for q in mxus]
    refs = [tile[0]] * pieces + [tile[1]] * pieces
    refs += [pltpu.ACC(q)((rest, TILE), F32) for q in mxus]
    refs += [pltpu.ACC(q)((early, TILE), F32) for q in mxus]
    pl.run_scoped(scoped, *refs)


def body(pred_input, proj_weight, proj_bias, targets, block_masks):
    images, patches, width = pred_input.shape
    feat = targets.shape[2]
    rows = proj_weight.shape[0]
    blocks = block_masks.shape[1]
    ndp, nmp = lax.axis_size("dp"), lax.axis_size("mp")
    ntot = ndp * nmp
    featp = pad_to(feat, LANES)
    groups = images // GROUP
    halves, parts = patches // LANES, width // LANES
    early = LANES
    rest = feat - early
    dma = pltpu.SemaphoreType.DMA
    vmem = pl.BlockSpec(memory_space=pltpu.VMEM)
    hbm = pl.BlockSpec(memory_space=pl.ANY)
    _, _, late_at, total_rows = layout(rows)
    inner_dp = 2
    outer_dp = ndp // inner_dp
    exchange = []
    for n in (late_at, total_rows - late_at):
        exchange += [
            pltpu.VMEM((inner_dp, outer_dp, n, LANES), F32),
            pltpu.VMEM((outer_dp, n, LANES), F32),
            pltpu.VMEM((outer_dp - 1, n, LANES), F32),
            pltpu.VMEM((outer_dp - 1, n, LANES), F32),
        ]
    exchange_sems = [dma(()), dma((outer_dp,)), dma(()), dma(())]
    summed = pl.pallas_call(
        functools.partial(kernel, ndp, nmp),
        out_shape=jax.ShapeDtypeStruct((total_rows + 8, LANES), F32),
        in_specs=[hbm] * 5,
        out_specs=hbm,
        scratch_shapes=[
            pltpu.VMEM((parts, images * patches, LANES), BF16),
            pltpu.VMEM((images, halves, feat, LANES), BF16),
            pltpu.VMEM((images, blocks, patches), jnp.int32),
            pltpu.VMEM((rows, feat), BF16),
            pltpu.VMEM((feat,), F32),
            pltpu.VMEM((total_rows + 8, LANES), F32),
            pltpu.VMEM((ndp, rows, feat), BF16),
            pltpu.VMEM((width, featp), F32),
            pltpu.VMEM((feat, pad_to(width, TILE)), BF16),
            pltpu.VMEM((patches, LANES), BF16),
            pltpu.VMEM((featp, LANES), F32),
            pltpu.VMEM((8, featp), F32),
            pltpu.VMEM((groups, 2 * GROUP, patches), F32),
            pltpu.VMEM((nmp - 1, groups, 2 * GROUP, patches), F32),
            pltpu.VMEM((images, patches), F32),
            pltpu.VMEM((images, patches), F32),
            pltpu.VMEM((images, patches), F32),
            pltpu.VMEM((PAIR, feat, patches), F32),
            pltpu.VMEM((PAIR, feat, patches), F32),
            pltpu.VMEM((rest, PAIR * patches), BF16),
            pltpu.VMEM((rest, PAIR * patches), BF16),
            pltpu.VMEM((images, halves, early, LANES), BF16),
            pltpu.VMEM((pad_to(rest, LANES), width), F32),
            pltpu.VMEM((early, width), F32),
            pltpu.VMEM((featp, LANES), F32),
            pltpu.VMEM((CHUNK, LANES), F32),
        ] + exchange + [
            pltpu.VMEM((1, LANES), F32),
            pltpu.VMEM((ntot, 1, LANES), F32),
            dma((groups,)), dma((groups,)), dma((2,)), dma(()), dma((2,)),
            dma(()), dma((outer_dp,)), dma(()), dma(()), dma(()), dma((groups,)),
        ] + exchange_sems * 2 + [dma(()), dma(())],
        compiler_params=pltpu.CompilerParams(
            collective_id=0, has_side_effects=True, vmem_limit_bytes=60 * 1024 * 1024
        ),
    )(
        pred_input.reshape(images * patches, width),
        proj_weight,
        proj_bias,
        jnp.swapaxes(targets, 1, 2),
        block_masks,
    )
    loss, clip, gw, gb = pl.pallas_call(
        functools.partial(finish, ndp, nmp),
        out_shape=(
            jax.ShapeDtypeStruct((1, 1), F32),
            jax.ShapeDtypeStruct((1, 1), F32),
            jax.ShapeDtypeStruct((rows, feat), F32),
            jax.ShapeDtypeStruct((feat,), F32),
        ),
        in_specs=[vmem],
        out_specs=(vmem,) * 4,
    )(summed)
    return loss.reshape(()), clip.reshape(()), gw, gb


def solution(mesh):
    in_specs = (
        P("dp", None, None),
        P("dp", "mp"),
        P("mp"),
        P("dp", None, "mp"),
        P("dp", None, None),
    )
    out_specs = (P(), P(), P("dp", "mp"), P("mp"))
    return jax.shard_map(body, mesh=mesh, in_specs=in_specs, out_specs=out_specs, check_vma=False)
```

```python
import functools

import jax
import jax.numpy as jnp
from jax import lax
from jax.experimental import pallas as pl
from jax.experimental.pallas import tpu as pltpu
from jax.sharding import PartitionSpec as P

F32 = jnp.float32
BF16 = jnp.bfloat16
MESH = pl.DeviceIdType.MESH
LANES = 128
GROUP = 8
PAIR = 2
CHUNK = 16
TILE = 256
ROWS = 32
SWEEP = 16
HANDS = (3, 5, 7)


def pad_to(n, m):
    return (n + m - 1) // m * m


def layout(rows):
    half = pad_to(rows, 8)
    sums = half + pad_to(rows // 2, 8)
    late = sums + 8
    return half, sums, late, late + pad_to(rows, 8)


def finish(ndp, nmp, sum_ref, loss_ref, clip_ref, gw_ref, gb_ref):
    rows, feat = gw_ref.shape
    half_at, sums_at, late_at, fin_at = layout(rows)
    tiles = pad_to(feat, LANES) // LANES
    count = sum_ref[sums_at + tiles + 1:sums_at + tiles + 2, 0:1]
    square, loss = sum_ref[fin_at:fin_at + 1, 0:1], sum_ref[fin_at:fin_at + 1, 1:2]
    norm = jnp.sqrt(square) / count
    scale = jnp.minimum(1.0, 1.0 / (norm + 1e-06))
    factor = scale / count
    loss_ref[...] = loss / count * (1.0 / (feat * nmp * ndp))
    clip_ref[...] = scale
    gw_ref[:, :LANES] = sum_ref[late_at:late_at + rows, :] * factor
    gw_ref[:, LANES:2 * LANES] = sum_ref[:rows, :] * factor
    half = LANES // 2
    packed = sum_ref[half_at:half_at + rows // 2, :] * factor
    gw_ref[:rows // 2, 2 * LANES:] = packed[:, :half]
    gw_ref[rows // 2:, 2 * LANES:] = packed[:, half:]
    for n in range(tiles):
        stop = min((n + 1) * LANES, feat)
        bias = sum_ref[sums_at + n:sums_at + n + 1, :] * factor
        gb_ref[n * LANES:stop] = bias[0, :stop - n * LANES]


def kernel(ndp, nmp, x_hbm, w_hbm, b_hbm, t_hbm, m_hbm,
           outv,
           xv, tv, mv, w_ref, b_ref, wall, wfull, wt, ones, bcol, brow, ssend, srecv, rbuf, mbuf, cbuf,
           pa, pb, sa, sb, s2, acc1, acc2, gacc, lacc,
           gs1, pv1, gm1, gr1, gs2, pv2, gm2, gr2, fsend, frecv,
           xsem, tsem, msem, bsem, wss, wrs, whs, whr, sss, srs, ps1, pr1, g1s, g1r, ps2, pr2, g2s, g2r, fss, frs):
    images, halves, feat, _ = tv.shape
    patches = halves * LANES
    parts, _, _ = xv.shape
    width = parts * LANES
    rows = w_ref.shape[0]
    early = s2.shape[2]
    rest = feat - early
    pieces = feat // ROWS
    dp, mp = lax.axis_index("dp"), lax.axis_index("mp")
    inner_dp, outer_dp = gs1.shape[0], gs1.shape[1]
    near, far = lax.rem(dp, inner_dp), dp // inner_dp
    featp = bcol.shape[0]
    groups = images // GROUP
    steps = images // PAIR
    ntot = ndp * nmp
    me = dp * nmp + mp
    feat_full = feat * nmp
    mxus = range(2)

    def scoped(*accs):
        proj = [list(accs[q * pieces:(q + 1) * pieces]) for q in mxus]
        grad_acc = list(accs[2 * pieces:2 * pieces + 2])
        late_acc = list(accs[2 * pieces + 2:2 * pieces + 4])

        def t_copy(g, h):
            s = pl.ds(g * GROUP, GROUP)
            return pltpu.make_async_copy(t_hbm.at[s, :, pl.ds(h * LANES, LANES)], tv.at[s, h], tsem.at[g])

        def x_copy(g, j):
            s = pl.ds(g * GROUP * patches, GROUP * patches)
            return pltpu.make_async_copy(x_hbm.at[s, pl.ds(j * LANES, LANES)], xv.at[j, s], xsem.at[g])

        def x_start(g):
            for j in range(parts):
                x_copy(g, j).start()

        def arrive(ref, sem):
            pltpu.make_async_copy(ref, ref, sem).wait()

        def x_wait(g):
            arrive(xv.at[:, pl.ds(g * GROUP * patches, GROUP * patches)], xsem.at[g])

        m_copy = pltpu.make_async_copy(m_hbm, mv, msem.at[0])
        w_own = pltpu.make_async_copy(w_hbm, w_ref, msem.at[1])
        b_own = pltpu.make_async_copy(b_hbm, b_ref, bsem)
        barrier = pltpu.get_barrier_semaphore()

        other = 1 - near

        def line(o):
            return lax.rem(far + o, outer_dp) * inner_dp + near

        partner = far * inner_dp + other
        peers = [(line(o), mp) for o in range(1, outer_dp)] + [(partner, mp)]
        peers += [(dp, lax.rem(mp + o, nmp)) for o in range(1, nmp)]
        for peer in peers:
            pl.semaphore_signal(barrier, inc=1, device_id=peer, device_id_type=MESH)
        w_own.start()
        b_own.start()
        m_copy.start()
        for g in range(groups):
            for h in range(halves):
                t_copy(g, h).start()

        pl.semaphore_wait(barrier, len(peers))

        def w_copy(o):
            return pltpu.make_async_remote_copy(
                src_ref=w_ref, dst_ref=wall.at[dp], send_sem=wss, recv_sem=wrs.at[o],
                device_id=(line(o), mp), device_id_type=MESH)

        def w_hand(o):
            src = lax.rem(far - o + outer_dp, outer_dp) * inner_dp + near
            own = isinstance(o, int) and o == 0
            return pltpu.make_async_remote_copy(
                src_ref=w_ref if own else wall.at[src], dst_ref=wall.at[src], send_sem=whs, recv_sem=whr,
                device_id=(partner, mp), device_id_type=MESH)

        def ranked(offset, n):
            picks = 0
            for f in range(outer_dp):
                near_first = sorted(range(1, outer_dp), key=lambda o: abs((f + offset * o) % outer_dp - f))
                picks = picks + jnp.where(far == f, near_first[n], 0)
            return picks

        w_own.wait()
        for n in reversed(range(outer_dp - 1)):
            w_copy(ranked(1, n)).start()
        w_hand(0).start()

        gacc[...] = jnp.zeros_like(gacc)
        lacc[...] = jnp.zeros_like(lacc)
        sb[...] = jnp.zeros_like(sb)
        acc1[...] = jnp.zeros_like(acc1)
        wfull[...] = jnp.zeros_like(wfull)
        brow[...] = jnp.zeros_like(brow)
        if rows % 16:
            gs1[...] = jnp.zeros_like(gs1)
            gs2[...] = jnp.zeros_like(gs2)
        lane = lax.broadcasted_iota(jnp.int32, ones.shape, 1)
        ones[...] = jnp.where(lane < 3, 1.0, 0.0).astype(BF16)
        b_own.wait()
        brow[0:1, :feat] = b_ref[...].reshape(1, feat)
        bcol[...] = jnp.transpose(jnp.broadcast_to(brow[0:1, :], (LANES, featp)))
        bias = bcol[:feat, :]
        high = bias.astype(BF16)
        left = bias - high.astype(F32)
        mid = left.astype(BF16)
        low = (left - mid.astype(F32)).astype(BF16)
        lane = lax.broadcasted_iota(jnp.int32, (feat, LANES), 1)
        pick = jnp.where(lane == 0, high.astype(F32), jnp.where(lane == 1, mid.astype(F32), low.astype(F32)))
        wt[:, width:] = jnp.where(lane < 3, pick, 0.0).astype(BF16)
        for q in mxus:
            blank = jnp.zeros((ROWS, TILE), BF16)
            pltpu.matmul_acc_lhs(proj[q][0], blank, load_staged_rhs=0)
            pltpu.matmul_acc_lhs(proj[q][0], blank, load_staged_rhs=1)
            for ref in proj[q] + [grad_acc[q], late_acc[q]]:
                pltpu.matmul_pop(ref)

        def x_tile(img, part):
            at = pl.ds(pl.multiple_of(img * patches, patches), patches)
            left = xv[2 * part, at, :]
            right = xv[2 * part + 1, at, :] if 2 * part + 1 < parts else ones[...]
            return jnp.concatenate([left, right], axis=1)

        def push_project(k, part):
            for q in mxus:
                tile = x_tile(PAIR * k + q, part)
                pltpu.matmul_push_rhs(tile, staging_register=part, mxu_index=q, transpose=True)

        def s_copy(o, g):
            return pltpu.make_async_remote_copy(
                src_ref=ssend.at[g], dst_ref=srecv.at[o - 1, g],
                send_sem=sss, recv_sem=srs.at[g],
                device_id=(dp, lax.rem(mp + o, nmp)), device_id_type=MESH)

        m_copy.wait()

        def cover(g, _):
            block = [jnp.sum(mv[g * GROUP + j], axis=0, keepdims=True) for j in range(GROUP)]
            cbuf[pl.ds(pl.multiple_of(g * GROUP, GROUP), GROUP), :] = jnp.concatenate(block, axis=0).astype(F32)
            return 0

        lax.fori_loop(0, groups, cover, 0)

        def stats(g, _):
            arrive(tv.at[pl.ds(g * GROUP, GROUP)], tsem.at[g])

            @pl.when(g >= 2)
            def _():
                x_start(g - 2)

            sums, squares = [], []
            for j in range(GROUP):
                i = g * GROUP + j
                for h in range(halves):
                    part = jnp.zeros((CHUNK, LANES), F32)
                    for c in range(0, feat, CHUNK):
                        part = part + tv[i, h, c:c + CHUNK, :].astype(F32)
                    total = jnp.sum(part, axis=0, keepdims=True)
                    mean = total * (1.0 / feat)
                    part = jnp.zeros((CHUNK, LANES), F32)
                    for c in range(0, feat, CHUNK):
                        centred = tv[i, h, c:c + CHUNK, :].astype(F32) - mean
                        part = part + centred * centred
                    sums.append(total)
                    squares.append(jnp.sum(part, axis=0, keepdims=True))
            for h in range(halves):
                block = jnp.concatenate(sums[h::halves] + squares[h::halves], axis=0)
                ssend[g, :, h * LANES:(h + 1) * LANES] = block

            @pl.when(g > 0)
            def _():
                for o in range(1, nmp):
                    s_copy(o, g - 1).start()

            for n in range(min(outer_dp - 1, len(HANDS))):
                pl.when(g == HANDS[n])(functools.partial(hand_over, n))

            return 0

        def hand_over(n):
            o = ranked(-1, n)
            w_copy(o).wait_recv()
            w_hand(o).start()

        lax.fori_loop(0, groups, stats, 0)
        for g in range(groups - 2, groups):
            x_start(g)

        for o in range(1, nmp):
            s_copy(o, groups - 1).start()
        for n in range(len(HANDS), outer_dp - 1):
            hand_over(n)
        x_wait(0)
        for part in range(2):
            push_project(0, part)
        wall[dp] = w_ref[...]
        arrive(wall.at[pl.ds(0, outer_dp)], whr)
        for k in range(ndp):
            wfull[k * rows:(k + 1) * rows, :feat] = wall[k].astype(F32)
        wt[:, :width] = jnp.transpose(wfull[...])[:feat].astype(BF16)

        def project(part, c):
            lhs = wt[c * ROWS:(c + 1) * ROWS, part * TILE:(part + 1) * TILE]
            for q in mxus:
                pltpu.matmul_acc_lhs(proj[q][c], lhs, load_staged_rhs=part if c == 0 else None)

        def push_gradient(k, g):
            for q in mxus:
                pltpu.matmul_push_rhs(x_tile(PAIR * k + g, q), staging_register=g, mxu_index=q)

        def gradient(s_ref, g):
            lhs = s_ref[:, g * patches:(g + 1) * patches]
            for q in mxus:
                pltpu.matmul_acc_lhs(grad_acc[q], lhs, load_staged_rhs=g)

        def keep(p_ref, c):
            for q in mxus:
                p_ref[q, c * ROWS:(c + 1) * ROWS, :] = pltpu.matmul_pop(proj[q][c])

        def pointwise(p_ref, s_ref, k, c, stat, loss):
            for f in range(c * ROWS, (c + 1) * ROWS, CHUNK):
                total = jnp.zeros((CHUNK, LANES), F32)
                for g in range(PAIR):
                    for h in range(halves):
                        lanes = slice(h * LANES, (h + 1) * LANES)
                        r, m, cov = [v[:, lanes] for v in stat[g]]
                        t = tv[PAIR * k + g, h, f:f + CHUNK, :].astype(F32)
                        differ = p_ref[g, f:f + CHUNK, lanes] + (m - t * r)
                        clipped = jnp.clip(differ, -1.0, 1.0)
                        source = clipped * cov
                        loss[h] = loss[h] + source * (differ - 0.5 * clipped)
                        total = total + source
                        if f < early:
                            s2[PAIR * k + g, h, f:f + CHUNK, :] = source.astype(BF16)
                        else:
                            at = g * patches + h * LANES
                            s_ref[f - early:f - early + CHUNK, at:at + LANES] = source.astype(BF16)
                gacc[f:f + CHUNK, :] += total

        def step(k, p_in, p_out, s_out, s_in):
            last = steps - 1
            back, ahead, beyond = jnp.maximum(k - 1, 0), jnp.minimum(k + 1, last), jnp.minimum(k + 2, last)
            stat = [[v[pl.ds(PAIR * k + g, 1), :] for v in (rbuf, mbuf, cbuf)] for g in range(PAIR)]
            loss = [jnp.zeros((CHUNK, LANES), F32)] * halves
            todo = [functools.partial(project, 0, c) for c in range(pieces)]
            todo.append(functools.partial(push_project, ahead, 1))
            todo += [functools.partial(project, 1, c) for c in range(pieces)]
            todo.append(functools.partial(push_gradient, back, 0))
            todo.append(functools.partial(gradient, s_in, 0))
            todo.append(functools.partial(push_gradient, back, 1))
            todo.append(functools.partial(push_project, beyond, 0))
            todo.append(functools.partial(gradient, s_in, 1))
            done = 0
            for c in range(pieces):
                upto = min(len(todo), pl.cdiv(len(todo) * (c + 1), pieces))
                for op in todo[done:upto]:
                    op()
                done = upto
                pointwise(p_in, s_out, k, c, stat, loss)
            for c in range(pieces):
                keep(p_out, c)
            lacc[...] += functools.reduce(jnp.add, loss)

        for part in range(2):
            for c in range(pieces):
                project(part, c)
        push_project(1, 0)
        for c in range(pieces):
            keep(pa, c)
        per_group = GROUP // PAIR

        def outer(g, _):
            @pl.when(g + 1 < groups)
            def _():
                x_wait(g + 1)

            arrive(srecv.at[:, g], srs.at[g])
            parts_in = [ssend[g]] + [srecv[o - 1, g] for o in range(1, nmp)]
            sums = [p[:GROUP] for p in parts_in]
            mean = functools.reduce(jnp.add, sums) * (1.0 / feat_full)
            var = functools.reduce(jnp.add, [p[GROUP:] for p in parts_in])
            for s in sums:
                gap = s * (1.0 / feat) - mean
                var = var + feat * (gap * gap)
            rstd = lax.rsqrt(var * (1.0 / feat_full) + 1e-05)
            here = pl.ds(pl.multiple_of(g * GROUP, GROUP), GROUP)
            rbuf[here, :] = rstd
            mbuf[here, :] = mean * rstd

            def inner(j, _):
                k = g * per_group + 2 * j
                step(k, pa, pb, sa, sb)
                pl.delay(1)
                step(k + 1, pb, pa, sb, sa)
                return 0

            lax.fori_loop(0, per_group // 2, inner, 0)
            return 0

        lax.fori_loop(0, groups, outer, 0)
        project(0, 0)
        for q in mxus:
            pltpu.matmul_pop(proj[q][0])
        for g in range(PAIR):
            push_gradient(steps - 1, g)
            gradient(sb, g)
        acc1[:rest, :TILE] = pltpu.matmul_pop(grad_acc[0])
        acc1[:rest, TILE:] = pltpu.matmul_pop(grad_acc[1])[:, :width - TILE]

        half_at, sums_at, late_at, total_rows = layout(rows)
        tiles = featp // LANES
        bias_part = jnp.sum(jnp.transpose(gacc[...]), axis=0, keepdims=True)
        loss_part = jnp.sum(lacc[...], keepdims=True)
        count_part = jnp.sum(cbuf[...], keepdims=True)
        at_row = lax.broadcasted_iota(jnp.int32, (8, LANES), 0)
        extra = jnp.where(at_row == tiles, loss_part, count_part)
        for n in range(tiles):
            extra = jnp.where(at_row == n, bias_part[:, n * LANES:(n + 1) * LANES], extra)
        full = jnp.transpose(acc1[...])
        half = LANES // 2
        for k in range(ndp):
            slot = gs1.at[k % inner_dp, k // inner_dp]
            mine = full[k * rows:(k + 1) * rows]
            slot[:rows, :] = mine[:, :LANES]
            slot[half_at:half_at + rows // 2, :] = jnp.concatenate(
                [mine[:rows // 2, LANES:LANES + half], mine[rows // 2:, LANES:LANES + half]], axis=1)
            slot[sums_at:, :] = extra

        def p_copy(o, bufs):
            src, dst, _, _, ss, rs, _, _ = bufs
            to = lax.rem(far + o, outer_dp)
            return pltpu.make_async_remote_copy(
                src_ref=src.at[other, to], dst_ref=dst.at[o], send_sem=ss, recv_sem=rs.at[o],
                device_id=(partner, mp), device_id_type=MESH)

        def g_copy(o, bufs):
            _, _, src, dst, _, _, ss, rs = bufs
            return pltpu.make_async_remote_copy(
                src_ref=src.at[o - 1], dst_ref=dst.at[o - 1], send_sem=ss, recv_sem=rs,
                device_id=(line(o), mp), device_id_type=MESH)

        first = (gs1, pv1, gm1, gr1, ps1, pr1, g1s, g1r)
        second = (gs2, pv2, gm2, gr2, ps2, pr2, g2s, g2r)
        order = [ranked(1, n) for n in reversed(range(outer_dp - 1))] + [0]
        for o in order:
            p_copy(o, first).start()

        def push_late(img, r):
            for q in mxus:
                pltpu.matmul_push_rhs(x_tile(img, q), staging_register=r, mxu_index=q)

        push_late(0, 0)

        def sweep(k, _):
            for g in range(SWEEP):
                img = k * SWEEP + g
                push_late(jnp.minimum(img + 1, images - 1), (g + 1) % 2)
                lhs = jnp.concatenate([s2[img, h, :, :] for h in range(halves)], axis=1)
                for q in mxus:
                    pltpu.matmul_acc_lhs(late_acc[q], lhs, load_staged_rhs=g % 2)
            return 0

        lax.fori_loop(0, images // SWEEP, sweep, 0)
        acc2[:, :TILE] = pltpu.matmul_pop(late_acc[0])
        acc2[:, TILE:] = pltpu.matmul_pop(late_acc[1])[:, :width - TILE]
        for q in mxus:
            pltpu.matmul_acc_lhs(late_acc[q], jnp.zeros((early, TILE), BF16), load_staged_rhs=0)
            pltpu.matmul_pop(late_acc[q])
        full = jnp.transpose(acc2[...])
        for k in range(ndp):
            gs2[k % inner_dp, k // inner_dp, :rows, :] = full[k * rows:(k + 1) * rows]
        for o in order:
            p_copy(o, second).start()

        pairs = []
        for bufs in (first, second):
            src, dst, mid_buf = bufs[:3]
            for o in order:
                p_copy(o, bufs).wait_recv()
                pair = src[near, lax.rem(far + o, outer_dp)] + dst[o]
                if o is not order[-1]:
                    mid_buf[o - 1] = pair
                    g_copy(o, bufs).start()
            pairs.append(pair)
        for n, bufs in enumerate((first, second)):
            arrive(bufs[3], bufs[7])
            for o in range(1, outer_dp):
                pairs[n] = pairs[n] + bufs[3][o - 1]
        outv[:late_at, :] = pairs[0]
        outv[late_at:total_rows, :] = pairs[1]
        head = pairs[0][:sums_at]
        sums = pairs[0][sums_at:]
        bias_grad = sums[:tiles]
        square = jnp.sum(head * head, keepdims=True) + jnp.sum(pairs[1] * pairs[1], keepdims=True)
        bias_square = jnp.sum(bias_grad * bias_grad, keepdims=True)
        lane = lax.broadcasted_iota(jnp.int32, (1, LANES), 1)
        fsend[...] = jnp.where(lane == 0, square + bias_square * (1.0 / ndp), sums[tiles:tiles + 1, :])

        def f_copy(d):
            return pltpu.make_async_remote_copy(
                src_ref=fsend, dst_ref=frecv.at[me], send_sem=fss, recv_sem=frs,
                device_id=(d // nmp, lax.rem(d, nmp)), device_id_type=MESH)

        def f_start(o, _):
            f_copy(o + jnp.where(o >= me, 1, 0)).start()
            return 0

        lax.fori_loop(0, ntot - 1, f_start, 0)
        frecv[me] = fsend[...]
        arrive(wall.at[pl.ds(0, outer_dp - 1)], wss)
        arrive(wall.at[pl.ds(0, outer_dp)], whs)
        for bufs in (first, second):
            arrive(bufs[0].at[0], bufs[4])
            arrive(bufs[2], bufs[6])
        arrive(srecv, sss)
        everyone = frecv.at[pl.ds(0, ntot - 1)]
        arrive(everyone, frs)
        outv[total_rows:, :] = jnp.broadcast_to(jnp.sum(frecv[...], axis=0), (8, LANES))
        arrive(everyone, fss)

    tile = [pltpu.ACC(q)((ROWS, TILE), F32) for q in mxus]
    refs = [tile[0]] * pieces + [tile[1]] * pieces
    refs += [pltpu.ACC(q)((rest, TILE), F32) for q in mxus]
    refs += [pltpu.ACC(q)((early, TILE), F32) for q in mxus]
    pl.run_scoped(scoped, *refs)


def body(pred_input, proj_weight, proj_bias, targets, block_masks):
    images, patches, width = pred_input.shape
    feat = targets.shape[2]
    rows = proj_weight.shape[0]
    blocks = block_masks.shape[1]
    ndp, nmp = lax.axis_size("dp"), lax.axis_size("mp")
    ntot = ndp * nmp
    featp = pad_to(feat, LANES)
    groups = images // GROUP
    halves, parts = patches // LANES, width // LANES
    early = LANES
    rest = feat - early
    dma = pltpu.SemaphoreType.DMA
    vmem = pl.BlockSpec(memory_space=pltpu.VMEM)
    hbm = pl.BlockSpec(memory_space=pl.ANY)
    _, _, late_at, total_rows = layout(rows)
    inner_dp = 2
    outer_dp = ndp // inner_dp
    exchange = []
    for n in (late_at, total_rows - late_at):
        exchange += [
            pltpu.VMEM((inner_dp, outer_dp, n, LANES), F32),
            pltpu.VMEM((outer_dp, n, LANES), F32),
            pltpu.VMEM((outer_dp - 1, n, LANES), F32),
            pltpu.VMEM((outer_dp - 1, n, LANES), F32),
        ]
    exchange_sems = [dma(()), dma((outer_dp,)), dma(()), dma(())]
    summed = pl.pallas_call(
        functools.partial(kernel, ndp, nmp),
        out_shape=pltpu.VMEM((total_rows + 8, LANES), F32),
        in_specs=[hbm] * 5,
        out_specs=vmem,
        scratch_shapes=[
            pltpu.VMEM((parts, images * patches, LANES), BF16),
            pltpu.VMEM((images, halves, feat, LANES), BF16),
            pltpu.VMEM((images, blocks, patches), jnp.int32),
            pltpu.VMEM((rows, feat), BF16),
            pltpu.VMEM((feat,), F32),
            pltpu.VMEM((ndp, rows, feat), BF16),
            pltpu.VMEM((width, featp), F32),
            pltpu.VMEM((feat, pad_to(width, TILE)), BF16),
            pltpu.VMEM((patches, LANES), BF16),
            pltpu.VMEM((featp, LANES), F32),
            pltpu.VMEM((8, featp), F32),
            pltpu.VMEM((groups, 2 * GROUP, patches), F32),
            pltpu.VMEM((nmp - 1, groups, 2 * GROUP, patches), F32),
            pltpu.VMEM((images, patches), F32),
            pltpu.VMEM((images, patches), F32),
            pltpu.VMEM((images, patches), F32),
            pltpu.VMEM((PAIR, feat, patches), F32),
            pltpu.VMEM((PAIR, feat, patches), F32),
            pltpu.VMEM((rest, PAIR * patches), BF16),
            pltpu.VMEM((rest, PAIR * patches), BF16),
            pltpu.VMEM((images, halves, early, LANES), BF16),
            pltpu.VMEM((pad_to(rest, LANES), width), F32),
            pltpu.VMEM((early, width), F32),
            pltpu.VMEM((featp, LANES), F32),
            pltpu.VMEM((CHUNK, LANES), F32),
        ] + exchange + [
            pltpu.VMEM((1, LANES), F32),
            pltpu.VMEM((ntot, 1, LANES), F32),
            dma((groups,)), dma((groups,)), dma((2,)), dma(()),
            dma(()), dma((outer_dp,)), dma(()), dma(()), dma(()), dma((groups,)),
        ] + exchange_sems * 2 + [dma(()), dma(())],
        compiler_params=pltpu.CompilerParams(
            collective_id=0, has_side_effects=True, vmem_limit_bytes=60 * 1024 * 1024
        ),
    )(
        pred_input.reshape(images * patches, width),
        proj_weight,
        proj_bias,
        jnp.swapaxes(targets, 1, 2),
        block_masks,
    )
    loss, clip, gw, gb = pl.pallas_call(
        functools.partial(finish, ndp, nmp),
        out_shape=(
            jax.ShapeDtypeStruct((1, 1), F32),
            jax.ShapeDtypeStruct((1, 1), F32),
            jax.ShapeDtypeStruct((rows, feat), F32),
            jax.ShapeDtypeStruct((feat,), F32),
        ),
        in_specs=[vmem],
        out_specs=(vmem,) * 4,
    )(pltpu.with_memory_space_constraint(summed, pltpu.VMEM))
    return loss.reshape(()), clip.reshape(()), gw, gb


def solution(mesh):
    in_specs = (
        P("dp", None, None),
        P("dp", "mp"),
        P("mp"),
        P("dp", None, "mp"),
        P("dp", None, None),
    )
    out_specs = (P(), P(), P("dp", "mp"), P("mp"))
    return jax.shard_map(body, mesh=mesh, in_specs=in_specs, out_specs=out_specs, check_vma=False)
```

```python
import functools

import jax
import jax.numpy as jnp
from jax import lax
from jax.experimental import pallas as pl
from jax.experimental.pallas import tpu as pltpu
from jax.sharding import PartitionSpec as P

F32 = jnp.float32
BF16 = jnp.bfloat16
MESH = pl.DeviceIdType.MESH
LANES = 128
GROUP = 8
PAIR = 2
CHUNK = 16
TILE = 256
ROWS = 32
SWEEP = 16
HANDS = (6, 7)


def pad_to(n, m):
    return (n + m - 1) // m * m


def layout(rows):
    half = pad_to(rows, 8)
    sums = half + pad_to(rows // 2, 8)
    late = sums + 8
    return half, sums, late, late + pad_to(rows, 8)


def finish(ndp, nmp, sum_ref, loss_ref, clip_ref, gw_ref, gb_ref):
    rows, feat = gw_ref.shape
    half_at, sums_at, late_at, fin_at = layout(rows)
    tiles = pad_to(feat, LANES) // LANES
    count = sum_ref[sums_at + tiles + 1:sums_at + tiles + 2, 0:1]
    square, loss = sum_ref[fin_at:fin_at + 1, 0:1], sum_ref[fin_at:fin_at + 1, 1:2]
    norm = jnp.sqrt(square) / count
    scale = jnp.minimum(1.0, 1.0 / (norm + 1e-06))
    factor = scale / count
    loss_ref[...] = loss / count * (1.0 / (feat * nmp * ndp))
    clip_ref[...] = scale
    gw_ref[:, :LANES] = sum_ref[late_at:late_at + rows, :] * factor
    gw_ref[:, LANES:2 * LANES] = sum_ref[:rows, :] * factor
    half = LANES // 2
    packed = sum_ref[half_at:half_at + rows // 2, :] * factor
    gw_ref[:rows // 2, 2 * LANES:] = packed[:, :half]
    gw_ref[rows // 2:, 2 * LANES:] = packed[:, half:]
    for n in range(tiles):
        stop = min((n + 1) * LANES, feat)
        bias = sum_ref[sums_at + n:sums_at + n + 1, :] * factor
        gb_ref[n * LANES:stop] = bias[0, :stop - n * LANES]


def kernel(ndp, nmp, x_hbm, w_hbm, b_hbm, t_hbm, m_hbm,
           outv,
           xv, tv, mv, w_ref, b_ref, wall, wfull, wt, ones, bcol, brow, ssend, srecv, rbuf, mbuf, cbuf,
           pa, pb, sa, sb, s2, acc1, acc2, gacc, lacc,
           gs1, pv1, gm1, gr1, gs2, pv2, gm2, gr2, fsend, frecv,
           xsem, tsem, msem, bsem, wss, wrs, whs, whr, sss, srs, ps1, pr1, g1s, g1r, ps2, pr2, g2s, g2r, fss, frs):
    images, halves, feat, _ = tv.shape
    patches = halves * LANES
    parts, _, _ = xv.shape
    width = parts * LANES
    rows = w_ref.shape[0]
    early = s2.shape[2]
    rest = feat - early
    pieces = feat // ROWS
    dp, mp = lax.axis_index("dp"), lax.axis_index("mp")
    inner_dp, outer_dp = gs1.shape[0], gs1.shape[1]
    near, far = lax.rem(dp, inner_dp), dp // inner_dp
    featp = bcol.shape[0]
    groups = images // GROUP
    steps = images // PAIR
    ntot = ndp * nmp
    me = dp * nmp + mp
    feat_full = feat * nmp
    mxus = range(2)

    def scoped(*accs):
        proj = [list(accs[q * pieces:(q + 1) * pieces]) for q in mxus]
        grad_acc = list(accs[2 * pieces:2 * pieces + 2])
        late_acc = list(accs[2 * pieces + 2:2 * pieces + 4])

        def t_copy(g, h):
            s = pl.ds(g * GROUP, GROUP)
            return pltpu.make_async_copy(t_hbm.at[s, :, pl.ds(h * LANES, LANES)], tv.at[s, h], tsem.at[g])

        def x_copy(g, j):
            s = pl.ds(g * GROUP * patches, GROUP * patches)
            return pltpu.make_async_copy(x_hbm.at[s, pl.ds(j * LANES, LANES)], xv.at[j, s], xsem.at[g])

        def x_start(g):
            for j in range(parts):
                x_copy(g, j).start()

        def arrive(ref, sem):
            pltpu.make_async_copy(ref, ref, sem).wait()

        def x_wait(g):
            arrive(xv.at[:, pl.ds(g * GROUP * patches, GROUP * patches)], xsem.at[g])

        m_copy = pltpu.make_async_copy(m_hbm, mv, msem.at[0])
        w_own = pltpu.make_async_copy(w_hbm, w_ref, msem.at[1])
        b_own = pltpu.make_async_copy(b_hbm, b_ref, bsem)
        barrier = pltpu.get_barrier_semaphore()

        other = 1 - near

        def line(o):
            return lax.rem(far + o, outer_dp) * inner_dp + near

        partner = far * inner_dp + other
        peers = [(line(o), mp) for o in range(1, outer_dp)] + [(partner, mp)]
        peers += [(dp, lax.rem(mp + o, nmp)) for o in range(1, nmp)]
        for peer in peers:
            pl.semaphore_signal(barrier, inc=1, device_id=peer, device_id_type=MESH)
        w_own.start()
        b_own.start()
        m_copy.start()
        for g in range(groups):
            for h in range(halves):
                t_copy(g, h).start()

        pl.semaphore_wait(barrier, len(peers))

        def w_copy(o):
            return pltpu.make_async_remote_copy(
                src_ref=w_ref, dst_ref=wall.at[dp], send_sem=wss, recv_sem=wrs.at[o],
                device_id=(line(o), mp), device_id_type=MESH)

        def w_hand(o):
            src = lax.rem(far - o + outer_dp, outer_dp) * inner_dp + near
            own = isinstance(o, int) and o == 0
            return pltpu.make_async_remote_copy(
                src_ref=w_ref if own else wall.at[src], dst_ref=wall.at[src], send_sem=whs, recv_sem=whr,
                device_id=(partner, mp), device_id_type=MESH)

        def ranked(offset, n):
            picks = 0
            for f in range(outer_dp):
                near_first = sorted(range(1, outer_dp), key=lambda o: abs((f + offset * o) % outer_dp - f))
                picks = picks + jnp.where(far == f, near_first[n], 0)
            return picks

        w_own.wait()
        for n in reversed(range(outer_dp - 1)):
            w_copy(ranked(1, n)).start()
        w_hand(0).start()

        def x_tile(img, part):
            at = pl.ds(pl.multiple_of(img * patches, patches), patches)
            left = xv[2 * part, at, :]
            right = xv[2 * part + 1, at, :] if 2 * part + 1 < parts else ones[...]
            return jnp.concatenate([left, right], axis=1)

        def push_project(k, part):
            for q in mxus:
                tile = x_tile(PAIR * k + q, part)
                pltpu.matmul_push_rhs(tile, staging_register=part, mxu_index=q, transpose=True)

        def s_copy(o, g):
            return pltpu.make_async_remote_copy(
                src_ref=ssend.at[g], dst_ref=srecv.at[o - 1, g],
                send_sem=sss, recv_sem=srs.at[g],
                device_id=(dp, lax.rem(mp + o, nmp)), device_id_type=MESH)

        def stats(g, _):
            arrive(tv.at[pl.ds(g * GROUP, GROUP)], tsem.at[g])

            @pl.when(g >= 2)
            def _():
                x_start(g - 2)

            sums, squares = [], []
            for j in range(GROUP):
                i = g * GROUP + j
                for h in range(halves):
                    part = jnp.zeros((CHUNK, LANES), F32)
                    for c in range(0, feat, CHUNK):
                        part = part + tv[i, h, c:c + CHUNK, :].astype(F32)
                    total = jnp.sum(part, axis=0, keepdims=True)
                    mean = total * (1.0 / feat)
                    part = jnp.zeros((CHUNK, LANES), F32)
                    for c in range(0, feat, CHUNK):
                        centred = tv[i, h, c:c + CHUNK, :].astype(F32) - mean
                        part = part + centred * centred
                    sums.append(total)
                    squares.append(jnp.sum(part, axis=0, keepdims=True))
            for h in range(halves):
                block = jnp.concatenate(sums[h::halves] + squares[h::halves], axis=0)
                ssend[g, :, h * LANES:(h + 1) * LANES] = block

            @pl.when(g > 0)
            def _():
                for o in range(1, nmp):
                    s_copy(o, g - 1).start()

            for n in range(min(outer_dp - 1, len(HANDS))):
                pl.when(g == HANDS[n])(functools.partial(hand_over, n))

            return 0

        def hand_over(n):
            src = n + jnp.where(n >= far, 1, 0)
            o = lax.rem(far - src + outer_dp, outer_dp)
            w_copy(o).wait_recv()
            w_hand(o).start()

        lax.fori_loop(0, groups, stats, 0)
        for g in range(groups - 2, groups):
            x_start(g)

        for o in range(1, nmp):
            s_copy(o, groups - 1).start()
        for n in range(len(HANDS), outer_dp - 1):
            hand_over(n)
        gacc[...] = jnp.zeros_like(gacc)
        lacc[...] = jnp.zeros_like(lacc)
        sb[...] = jnp.zeros_like(sb)
        acc1[...] = jnp.zeros_like(acc1)
        wfull[...] = jnp.zeros_like(wfull)
        brow[...] = jnp.zeros_like(brow)
        if rows % 16:
            gs1[...] = jnp.zeros_like(gs1)
            gs2[...] = jnp.zeros_like(gs2)
        lane = lax.broadcasted_iota(jnp.int32, ones.shape, 1)
        ones[...] = jnp.where(lane < 3, 1.0, 0.0).astype(BF16)
        b_own.wait()
        brow[0:1, :feat] = b_ref[...].reshape(1, feat)
        bcol[...] = jnp.transpose(jnp.broadcast_to(brow[0:1, :], (LANES, featp)))
        bias = bcol[:feat, :]
        high = bias.astype(BF16)
        left = bias - high.astype(F32)
        mid = left.astype(BF16)
        low = (left - mid.astype(F32)).astype(BF16)
        lane = lax.broadcasted_iota(jnp.int32, (feat, LANES), 1)
        pick = jnp.where(lane == 0, high.astype(F32), jnp.where(lane == 1, mid.astype(F32), low.astype(F32)))
        wt[:, width:] = jnp.where(lane < 3, pick, 0.0).astype(BF16)
        for q in mxus:
            blank = jnp.zeros((ROWS, TILE), BF16)
            pltpu.matmul_acc_lhs(proj[q][0], blank, load_staged_rhs=0)
            pltpu.matmul_acc_lhs(proj[q][0], blank, load_staged_rhs=1)
            for ref in proj[q] + [grad_acc[q], late_acc[q]]:
                pltpu.matmul_pop(ref)

        m_copy.wait()

        def cover(g, _):
            block = [jnp.sum(mv[g * GROUP + j], axis=0, keepdims=True) for j in range(GROUP)]
            cbuf[pl.ds(pl.multiple_of(g * GROUP, GROUP), GROUP), :] = jnp.concatenate(block, axis=0).astype(F32)
            return 0

        lax.fori_loop(0, groups, cover, 0)

        x_wait(0)
        for part in range(2):
            push_project(0, part)
        wall[dp] = w_ref[...]
        arrive(wall.at[pl.ds(0, outer_dp)], whr)
        for k in range(ndp):
            wfull[k * rows:(k + 1) * rows, :feat] = wall[k].astype(F32)
        wt[:, :width] = jnp.transpose(wfull[...])[:feat].astype(BF16)

        def project(part, c):
            lhs = wt[c * ROWS:(c + 1) * ROWS, part * TILE:(part + 1) * TILE]
            for q in mxus:
                pltpu.matmul_acc_lhs(proj[q][c], lhs, load_staged_rhs=part if c == 0 else None)

        def push_gradient(k, g):
            for q in mxus:
                pltpu.matmul_push_rhs(x_tile(PAIR * k + g, q), staging_register=g, mxu_index=q)

        def gradient(s_ref, g):
            lhs = s_ref[:, g * patches:(g + 1) * patches]
            for q in mxus:
                pltpu.matmul_acc_lhs(grad_acc[q], lhs, load_staged_rhs=g)

        def keep(p_ref, c):
            for q in mxus:
                p_ref[q, c * ROWS:(c + 1) * ROWS, :] = pltpu.matmul_pop(proj[q][c])

        def pointwise(p_ref, s_ref, k, c, stat, loss):
            for f in range(c * ROWS, (c + 1) * ROWS, CHUNK):
                total = jnp.zeros((CHUNK, LANES), F32)
                for g in range(PAIR):
                    for h in range(halves):
                        lanes = slice(h * LANES, (h + 1) * LANES)
                        r, m, cov = [v[:, lanes] for v in stat[g]]
                        t = tv[PAIR * k + g, h, f:f + CHUNK, :].astype(F32)
                        differ = p_ref[g, f:f + CHUNK, lanes] + (m - t * r)
                        clipped = jnp.clip(differ, -1.0, 1.0)
                        source = clipped * cov
                        loss[h] = loss[h] + source * (differ - 0.5 * clipped)
                        total = total + source
                        if f < early:
                            s2[PAIR * k + g, h, f:f + CHUNK, :] = source.astype(BF16)
                        else:
                            at = g * patches + h * LANES
                            s_ref[f - early:f - early + CHUNK, at:at + LANES] = source.astype(BF16)
                gacc[f:f + CHUNK, :] += total

        def step(k, p_in, p_out, s_out, s_in):
            last = steps - 1
            back, ahead, beyond = jnp.maximum(k - 1, 0), jnp.minimum(k + 1, last), jnp.minimum(k + 2, last)
            stat = [[v[pl.ds(PAIR * k + g, 1), :] for v in (rbuf, mbuf, cbuf)] for g in range(PAIR)]
            loss = [jnp.zeros((CHUNK, LANES), F32)] * halves
            todo = [functools.partial(project, 0, c) for c in range(pieces)]
            todo.append(functools.partial(push_project, ahead, 1))
            todo += [functools.partial(project, 1, c) for c in range(pieces)]
            todo.append(functools.partial(push_gradient, back, 0))
            todo.append(functools.partial(gradient, s_in, 0))
            todo.append(functools.partial(push_gradient, back, 1))
            todo.append(functools.partial(push_project, beyond, 0))
            todo.append(functools.partial(gradient, s_in, 1))
            done = 0
            for c in range(pieces):
                upto = min(len(todo), pl.cdiv(len(todo) * (c + 1), pieces))
                for op in todo[done:upto]:
                    op()
                done = upto
                pointwise(p_in, s_out, k, c, stat, loss)
            for c in range(pieces):
                keep(p_out, c)
            lacc[...] += functools.reduce(jnp.add, loss)

        for part in range(2):
            for c in range(pieces):
                project(part, c)
        push_project(1, 0)
        for c in range(pieces):
            keep(pa, c)
        per_group = GROUP // PAIR

        def outer(g, _):
            @pl.when(g + 1 < groups)
            def _():
                x_wait(g + 1)

            arrive(srecv.at[:, g], srs.at[g])
            parts_in = [ssend[g]] + [srecv[o - 1, g] for o in range(1, nmp)]
            sums = [p[:GROUP] for p in parts_in]
            mean = functools.reduce(jnp.add, sums) * (1.0 / feat_full)
            var = functools.reduce(jnp.add, [p[GROUP:] for p in parts_in])
            for s in sums:
                gap = s * (1.0 / feat) - mean
                var = var + feat * (gap * gap)
            rstd = lax.rsqrt(var * (1.0 / feat_full) + 1e-05)
            here = pl.ds(pl.multiple_of(g * GROUP, GROUP), GROUP)
            rbuf[here, :] = rstd
            mbuf[here, :] = mean * rstd

            def inner(j, _):
                k = g * per_group + 2 * j
                step(k, pa, pb, sa, sb)
                pl.delay(1)
                step(k + 1, pb, pa, sb, sa)
                return 0

            lax.fori_loop(0, per_group // 2, inner, 0)
            return 0

        lax.fori_loop(0, groups, outer, 0)
        project(0, 0)
        for q in mxus:
            pltpu.matmul_pop(proj[q][0])
        for g in range(PAIR):
            push_gradient(steps - 1, g)
            gradient(sb, g)
        acc1[:rest, :TILE] = pltpu.matmul_pop(grad_acc[0])
        acc1[:rest, TILE:] = pltpu.matmul_pop(grad_acc[1])[:, :width - TILE]

        half_at, sums_at, late_at, total_rows = layout(rows)
        tiles = featp // LANES
        bias_part = jnp.sum(jnp.transpose(gacc[...]), axis=0, keepdims=True)
        loss_part = jnp.sum(lacc[...], keepdims=True)
        count_part = jnp.sum(cbuf[...], keepdims=True)
        at_row = lax.broadcasted_iota(jnp.int32, (8, LANES), 0)
        extra = jnp.where(at_row == tiles, loss_part, count_part)
        for n in range(tiles):
            extra = jnp.where(at_row == n, bias_part[:, n * LANES:(n + 1) * LANES], extra)
        full = jnp.transpose(acc1[...])
        half = LANES // 2
        for k in range(ndp):
            slot = gs1.at[k % inner_dp, k // inner_dp]
            mine = full[k * rows:(k + 1) * rows]
            slot[:rows, :] = mine[:, :LANES]
            slot[half_at:half_at + rows // 2, :] = jnp.concatenate(
                [mine[:rows // 2, LANES:LANES + half], mine[rows // 2:, LANES:LANES + half]], axis=1)
            slot[sums_at:, :] = extra

        def p_copy(o, bufs):
            src, dst, _, _, ss, rs, _, _ = bufs
            to = lax.rem(far + o, outer_dp)
            return pltpu.make_async_remote_copy(
                src_ref=src.at[other, to], dst_ref=dst.at[o], send_sem=ss, recv_sem=rs.at[o],
                device_id=(partner, mp), device_id_type=MESH)

        def g_copy(o, bufs):
            _, _, src, dst, _, _, ss, rs = bufs
            return pltpu.make_async_remote_copy(
                src_ref=src.at[o - 1], dst_ref=dst.at[o - 1], send_sem=ss, recv_sem=rs,
                device_id=(line(o), mp), device_id_type=MESH)

        first = (gs1, pv1, gm1, gr1, ps1, pr1, g1s, g1r)
        second = (gs2, pv2, gm2, gr2, ps2, pr2, g2s, g2r)
        order = [ranked(1, n) for n in reversed(range(outer_dp - 1))] + [0]
        for o in order:
            p_copy(o, first).start()

        def push_late(img, r):
            for q in mxus:
                pltpu.matmul_push_rhs(x_tile(img, q), staging_register=r, mxu_index=q)

        push_late(0, 0)

        def sweep(k, _):
            for g in range(SWEEP):
                img = k * SWEEP + g
                push_late(jnp.minimum(img + 1, images - 1), (g + 1) % 2)
                lhs = jnp.concatenate([s2[img, h, :, :] for h in range(halves)], axis=1)
                for q in mxus:
                    pltpu.matmul_acc_lhs(late_acc[q], lhs, load_staged_rhs=g % 2)
            return 0

        lax.fori_loop(0, images // SWEEP, sweep, 0)
        acc2[:, :TILE] = pltpu.matmul_pop(late_acc[0])
        acc2[:, TILE:] = pltpu.matmul_pop(late_acc[1])[:, :width - TILE]
        for q in mxus:
            pltpu.matmul_acc_lhs(late_acc[q], jnp.zeros((early, TILE), BF16), load_staged_rhs=0)
            pltpu.matmul_pop(late_acc[q])
        full = jnp.transpose(acc2[...])
        for k in range(ndp):
            gs2[k % inner_dp, k // inner_dp, :rows, :] = full[k * rows:(k + 1) * rows]
        for o in order:
            p_copy(o, second).start()

        pairs = []
        for bufs in (first, second):
            src, dst, mid_buf = bufs[:3]
            for o in order:
                p_copy(o, bufs).wait_recv()
                pair = src[near, lax.rem(far + o, outer_dp)] + dst[o]
                if o is not order[-1]:
                    mid_buf[o - 1] = pair
                    g_copy(o, bufs).start()
            pairs.append(pair)
        for n, bufs in enumerate((first, second)):
            arrive(bufs[3], bufs[7])
            for o in range(1, outer_dp):
                pairs[n] = pairs[n] + bufs[3][o - 1]
        outv[:late_at, :] = pairs[0]
        outv[late_at:total_rows, :] = pairs[1]
        head = pairs[0][:sums_at]
        sums = pairs[0][sums_at:]
        bias_grad = sums[:tiles]
        square = jnp.sum(head * head, keepdims=True) + jnp.sum(pairs[1] * pairs[1], keepdims=True)
        bias_square = jnp.sum(bias_grad * bias_grad, keepdims=True)
        lane = lax.broadcasted_iota(jnp.int32, (1, LANES), 1)
        fsend[...] = jnp.where(lane == 0, square + bias_square * (1.0 / ndp), sums[tiles:tiles + 1, :])

        def f_copy(d):
            return pltpu.make_async_remote_copy(
                src_ref=fsend, dst_ref=frecv.at[me], send_sem=fss, recv_sem=frs,
                device_id=(d // nmp, lax.rem(d, nmp)), device_id_type=MESH)

        def f_start(o, _):
            f_copy(o + jnp.where(o >= me, 1, 0)).start()
            return 0

        lax.fori_loop(0, ntot - 1, f_start, 0)
        frecv[me] = fsend[...]
        arrive(wall.at[pl.ds(0, outer_dp - 1)], wss)
        arrive(wall.at[pl.ds(0, outer_dp)], whs)
        for bufs in (first, second):
            arrive(bufs[0].at[0], bufs[4])
            arrive(bufs[2], bufs[6])
        arrive(srecv, sss)
        everyone = frecv.at[pl.ds(0, ntot - 1)]
        arrive(everyone, frs)
        outv[total_rows:, :] = jnp.broadcast_to(jnp.sum(frecv[...], axis=0), (8, LANES))
        arrive(everyone, fss)

    tile = [pltpu.ACC(q)((ROWS, TILE), F32) for q in mxus]
    refs = [tile[0]] * pieces + [tile[1]] * pieces
    refs += [pltpu.ACC(q)((rest, TILE), F32) for q in mxus]
    refs += [pltpu.ACC(q)((early, TILE), F32) for q in mxus]
    pl.run_scoped(scoped, *refs)


def body(pred_input, proj_weight, proj_bias, targets, block_masks):
    images, patches, width = pred_input.shape
    feat = targets.shape[2]
    rows = proj_weight.shape[0]
    blocks = block_masks.shape[1]
    ndp, nmp = lax.axis_size("dp"), lax.axis_size("mp")
    ntot = ndp * nmp
    featp = pad_to(feat, LANES)
    groups = images // GROUP
    halves, parts = patches // LANES, width // LANES
    early = LANES
    rest = feat - early
    dma = pltpu.SemaphoreType.DMA
    vmem = pl.BlockSpec(memory_space=pltpu.VMEM)
    hbm = pl.BlockSpec(memory_space=pl.ANY)
    _, _, late_at, total_rows = layout(rows)
    inner_dp = 2
    outer_dp = ndp // inner_dp
    exchange = []
    for n in (late_at, total_rows - late_at):
        exchange += [
            pltpu.VMEM((inner_dp, outer_dp, n, LANES), F32),
            pltpu.VMEM((outer_dp, n, LANES), F32),
            pltpu.VMEM((outer_dp - 1, n, LANES), F32),
            pltpu.VMEM((outer_dp - 1, n, LANES), F32),
        ]
    exchange_sems = [dma(()), dma((outer_dp,)), dma(()), dma(())]
    summed = pl.pallas_call(
        functools.partial(kernel, ndp, nmp),
        out_shape=pltpu.VMEM((total_rows + 8, LANES), F32),
        in_specs=[hbm] * 5,
        out_specs=vmem,
        scratch_shapes=[
            pltpu.VMEM((parts, images * patches, LANES), BF16),
            pltpu.VMEM((images, halves, feat, LANES), BF16),
            pltpu.VMEM((images, blocks, patches), jnp.int32),
            pltpu.VMEM((rows, feat), BF16),
            pltpu.VMEM((feat,), F32),
            pltpu.VMEM((ndp, rows, feat), BF16),
            pltpu.VMEM((width, featp), F32),
            pltpu.VMEM((feat, pad_to(width, TILE)), BF16),
            pltpu.VMEM((patches, LANES), BF16),
            pltpu.VMEM((featp, LANES), F32),
            pltpu.VMEM((8, featp), F32),
            pltpu.VMEM((groups, 2 * GROUP, patches), F32),
            pltpu.VMEM((nmp - 1, groups, 2 * GROUP, patches), F32),
            pltpu.VMEM((images, patches), F32),
            pltpu.VMEM((images, patches), F32),
            pltpu.VMEM((images, patches), F32),
            pltpu.VMEM((PAIR, feat, patches), F32),
            pltpu.VMEM((PAIR, feat, patches), F32),
            pltpu.VMEM((rest, PAIR * patches), BF16),
            pltpu.VMEM((rest, PAIR * patches), BF16),
            pltpu.VMEM((images, halves, early, LANES), BF16),
            pltpu.VMEM((pad_to(rest, LANES), width), F32),
            pltpu.VMEM((early, width), F32),
            pltpu.VMEM((featp, LANES), F32),
            pltpu.VMEM((CHUNK, LANES), F32),
        ] + exchange + [
            pltpu.VMEM((1, LANES), F32),
            pltpu.VMEM((ntot, 1, LANES), F32),
            dma((groups,)), dma((groups,)), dma((2,)), dma(()),
            dma(()), dma((outer_dp,)), dma(()), dma(()), dma(()), dma((groups,)),
        ] + exchange_sems * 2 + [dma(()), dma(())],
        compiler_params=pltpu.CompilerParams(
            collective_id=0, has_side_effects=True, vmem_limit_bytes=60 * 1024 * 1024
        ),
    )(
        pred_input.reshape(images * patches, width),
        proj_weight,
        proj_bias,
        jnp.swapaxes(targets, 1, 2),
        block_masks,
    )
    loss, clip, gw, gb = pl.pallas_call(
        functools.partial(finish, ndp, nmp),
        out_shape=(
            jax.ShapeDtypeStruct((1, 1), F32),
            jax.ShapeDtypeStruct((1, 1), F32),
            jax.ShapeDtypeStruct((rows, feat), F32),
            jax.ShapeDtypeStruct((feat,), F32),
        ),
        in_specs=[vmem],
        out_specs=(vmem,) * 4,
    )(pltpu.with_memory_space_constraint(summed, pltpu.VMEM))
    return loss.reshape(()), clip.reshape(()), gw, gb


def solution(mesh):
    in_specs = (
        P("dp", None, None),
        P("dp", "mp"),
        P("mp"),
        P("dp", None, "mp"),
        P("dp", None, None),
    )
    out_specs = (P(), P(), P("dp", "mp"), P("mp"))
    return jax.shard_map(body, mesh=mesh, in_specs=in_specs, out_specs=out_specs, check_vma=False)
```

```python
import functools

import jax
import jax.numpy as jnp
from jax import lax
from jax.experimental import pallas as pl
from jax.experimental.pallas import tpu as pltpu
from jax.sharding import PartitionSpec as P

F32 = jnp.float32
BF16 = jnp.bfloat16
MESH = pl.DeviceIdType.MESH
LANES = 128
GROUP = 8
PAIR = 2
CHUNK = 16
TILE = 256
ROWS = 16
SWEEP = 32
HANDS = (6, 7)


def pad_to(n, m):
    return (n + m - 1) // m * m


def layout(rows):
    half = pad_to(rows, 8)
    sums = half + pad_to(rows // 2, 8)
    late = sums + 8
    return half, sums, late, late + pad_to(rows, 8)


def finish(ndp, nmp, sum_ref, loss_ref, clip_ref, gw_ref, gb_ref):
    rows, feat = gw_ref.shape
    half_at, sums_at, late_at, fin_at = layout(rows)
    tiles = pad_to(feat, LANES) // LANES
    count = sum_ref[sums_at + tiles + 1:sums_at + tiles + 2, 0:1]
    square, loss = sum_ref[fin_at:fin_at + 1, 0:1], sum_ref[fin_at:fin_at + 1, 1:2]
    norm = jnp.sqrt(square) / count
    scale = jnp.minimum(1.0, 1.0 / (norm + 1e-06))
    factor = scale / count
    loss_ref[...] = loss / count * (1.0 / (feat * nmp * ndp))
    clip_ref[...] = scale
    gw_ref[:, :LANES] = sum_ref[late_at:late_at + rows, :] * factor
    gw_ref[:, LANES:2 * LANES] = sum_ref[:rows, :] * factor
    half = LANES // 2
    packed = sum_ref[half_at:half_at + rows // 2, :] * factor
    gw_ref[:rows // 2, 2 * LANES:] = packed[:, :half]
    gw_ref[rows // 2:, 2 * LANES:] = packed[:, half:]
    for n in range(tiles):
        stop = min((n + 1) * LANES, feat)
        bias = sum_ref[sums_at + n:sums_at + n + 1, :] * factor
        gb_ref[n * LANES:stop] = bias[0, :stop - n * LANES]


def kernel(ndp, nmp, x_hbm, w_hbm, b_hbm, t_hbm, m_hbm,
           outv,
           xv, tv, mv, w_ref, b_ref, wall, wfull, wt, ones, bcol, brow, ssend, srecv, rbuf, mbuf, cbuf,
           pa, pb, sa, sb, s2, acc1, acc2, gacc, lacc,
           gs1, pv1, gm1, gr1, gs2, pv2, gm2, gr2, hs, hr, ht, hv, fsend, frecv,
           xsem, tsem, msem, bsem, wss, wrs, whs, whr, sss, srs, ps1, pr1, g1s, g1r, ps2, pr2, g2s, g2r, hss, hrs, hps, hpr, fss, frs):
    images, halves, feat, _ = tv.shape
    patches = halves * LANES
    parts, _, _ = xv.shape
    width = parts * LANES
    rows = w_ref.shape[0]
    early = s2.shape[2]
    rest = feat - early
    pieces = feat // ROWS
    dp, mp = lax.axis_index("dp"), lax.axis_index("mp")
    inner_dp, outer_dp = gs1.shape[0], gs1.shape[1]
    near, far = lax.rem(dp, inner_dp), dp // inner_dp
    featp = bcol.shape[0]
    groups = images // GROUP
    steps = images // PAIR
    ntot = ndp * nmp
    me = dp * nmp + mp
    feat_full = feat * nmp
    mxus = range(2)

    def scoped(*accs):
        proj = [list(accs[q * pieces:(q + 1) * pieces]) for q in mxus]
        grad_acc = list(accs[2 * pieces:2 * pieces + 2])
        late_acc = list(accs[2 * pieces + 2:2 * pieces + 4])

        def t_copy(g, h):
            s = pl.ds(g * GROUP, GROUP)
            return pltpu.make_async_copy(t_hbm.at[s, :, pl.ds(h * LANES, LANES)], tv.at[s, h], tsem.at[g])

        def x_copy(g, j):
            s = pl.ds(g * GROUP * patches, GROUP * patches)
            return pltpu.make_async_copy(x_hbm.at[s, pl.ds(j * LANES, LANES)], xv.at[j, s], xsem.at[g])

        def x_start(g):
            for j in range(parts):
                x_copy(g, j).start()

        def arrive(ref, sem):
            pltpu.make_async_copy(ref, ref, sem).wait()

        def x_wait(g):
            arrive(xv.at[:, pl.ds(g * GROUP * patches, GROUP * patches)], xsem.at[g])

        m_copy = pltpu.make_async_copy(m_hbm, mv, msem.at[0])
        w_own = pltpu.make_async_copy(w_hbm, w_ref, msem.at[1])
        b_own = pltpu.make_async_copy(b_hbm, b_ref, bsem)
        barrier = pltpu.get_barrier_semaphore()

        other = 1 - near

        def line(o):
            return lax.rem(far + o, outer_dp) * inner_dp + near

        partner = far * inner_dp + other
        peers = [(line(o), mp) for o in range(1, outer_dp)] + [(partner, mp)]
        peers += [(dp, lax.rem(mp + o, nmp)) for o in range(1, nmp)]
        for peer in peers:
            pl.semaphore_signal(barrier, inc=1, device_id=peer, device_id_type=MESH)
        w_own.start()
        b_own.start()
        m_copy.start()
        for g in range(groups):
            for h in range(halves):
                t_copy(g, h).start()

        pl.semaphore_wait(barrier, len(peers))

        def w_copy(o):
            return pltpu.make_async_remote_copy(
                src_ref=w_ref, dst_ref=wall.at[dp], send_sem=wss, recv_sem=wrs.at[o],
                device_id=(line(o), mp), device_id_type=MESH)

        def w_hand(o):
            src = lax.rem(far - o + outer_dp, outer_dp) * inner_dp + near
            own = isinstance(o, int) and o == 0
            return pltpu.make_async_remote_copy(
                src_ref=w_ref if own else wall.at[src], dst_ref=wall.at[src], send_sem=whs, recv_sem=whr,
                device_id=(partner, mp), device_id_type=MESH)

        def ranked(offset, n):
            picks = 0
            for f in range(outer_dp):
                near_first = sorted(range(1, outer_dp), key=lambda o: abs((f + offset * o) % outer_dp - f))
                picks = picks + jnp.where(far == f, near_first[n], 0)
            return picks

        w_own.wait()
        for n in reversed(range(outer_dp - 1)):
            w_copy(ranked(1, n)).start()
        w_hand(0).start()

        def x_tile(img, part):
            at = pl.ds(pl.multiple_of(img * patches, patches), patches)
            left = xv[2 * part, at, :]
            right = xv[2 * part + 1, at, :] if 2 * part + 1 < parts else ones[...]
            return jnp.concatenate([left, right], axis=1)

        def push_project(k, part):
            for q in mxus:
                tile = x_tile(PAIR * k + q, part)
                pltpu.matmul_push_rhs(tile, staging_register=part, mxu_index=q, transpose=True)

        def s_copy(o, g):
            return pltpu.make_async_remote_copy(
                src_ref=ssend.at[g], dst_ref=srecv.at[o - 1, g],
                send_sem=sss, recv_sem=srs.at[g],
                device_id=(dp, lax.rem(mp + o, nmp)), device_id_type=MESH)

        def stats(g, _):
            arrive(tv.at[pl.ds(g * GROUP, GROUP)], tsem.at[g])

            @pl.when(g >= 2)
            def _():
                x_start(g - 2)

            sums, squares = [], []
            for j in range(GROUP):
                i = g * GROUP + j
                for h in range(halves):
                    part = jnp.zeros((CHUNK, LANES), F32)
                    for c in range(0, feat, CHUNK):
                        part = part + tv[i, h, c:c + CHUNK, :].astype(F32)
                    total = jnp.sum(part, axis=0, keepdims=True)
                    mean = total * (1.0 / feat)
                    part = jnp.zeros((CHUNK, LANES), F32)
                    for c in range(0, feat, CHUNK):
                        centred = tv[i, h, c:c + CHUNK, :].astype(F32) - mean
                        part = part + centred * centred
                    sums.append(total)
                    squares.append(jnp.sum(part, axis=0, keepdims=True))
            for h in range(halves):
                block = jnp.concatenate(sums[h::halves] + squares[h::halves], axis=0)
                ssend[g, :, h * LANES:(h + 1) * LANES] = block

            @pl.when(g > 0)
            def _():
                for o in range(1, nmp):
                    s_copy(o, g - 1).start()

            for n in range(min(outer_dp - 1, len(HANDS))):
                pl.when(g == HANDS[n])(functools.partial(hand_over, n))

            return 0

        def hand_over(n):
            src = n + jnp.where(n >= far, 1, 0)
            o = lax.rem(far - src + outer_dp, outer_dp)
            w_copy(o).wait_recv()
            w_hand(o).start()

        lax.fori_loop(0, groups, stats, 0)
        for g in range(groups - 2, groups):
            x_start(g)

        for o in range(1, nmp):
            s_copy(o, groups - 1).start()
        for n in range(len(HANDS), outer_dp - 1):
            hand_over(n)
        gacc[...] = jnp.zeros_like(gacc)
        lacc[...] = jnp.zeros_like(lacc)
        sb[...] = jnp.zeros_like(sb)
        acc1[...] = jnp.zeros_like(acc1)
        wfull[...] = jnp.zeros_like(wfull)
        brow[...] = jnp.zeros_like(brow)
        if rows % 16:
            gs1[...] = jnp.zeros_like(gs1)
            gs2[...] = jnp.zeros_like(gs2)
            hs[...] = jnp.zeros_like(hs)
        lane = lax.broadcasted_iota(jnp.int32, ones.shape, 1)
        ones[...] = jnp.where(lane < 3, 1.0, 0.0).astype(BF16)
        b_own.wait()
        brow[0:1, :feat] = b_ref[...].reshape(1, feat)
        bcol[...] = jnp.transpose(jnp.broadcast_to(brow[0:1, :], (LANES, featp)))
        bias = bcol[:feat, :]
        high = bias.astype(BF16)
        left = bias - high.astype(F32)
        mid = left.astype(BF16)
        low = (left - mid.astype(F32)).astype(BF16)
        lane = lax.broadcasted_iota(jnp.int32, (feat, LANES), 1)
        pick = jnp.where(lane == 0, high.astype(F32), jnp.where(lane == 1, mid.astype(F32), low.astype(F32)))
        wt[:, width:] = jnp.where(lane < 3, pick, 0.0).astype(BF16)
        for q in mxus:
            blank = jnp.zeros((ROWS, TILE), BF16)
            pltpu.matmul_acc_lhs(proj[q][0], blank, load_staged_rhs=0)
            pltpu.matmul_acc_lhs(proj[q][0], blank, load_staged_rhs=1)
            for ref in proj[q] + [grad_acc[q], late_acc[q]]:
                pltpu.matmul_pop(ref)

        m_copy.wait()

        def cover(g, _):
            block = [jnp.sum(mv[g * GROUP + j], axis=0, keepdims=True) for j in range(GROUP)]
            cbuf[pl.ds(pl.multiple_of(g * GROUP, GROUP), GROUP), :] = jnp.concatenate(block, axis=0).astype(F32)
            return 0

        lax.fori_loop(0, groups, cover, 0)

        x_wait(0)
        for part in range(2):
            push_project(0, part)
        wall[dp] = w_ref[...]
        arrive(wall.at[pl.ds(0, outer_dp)], whr)
        for k in range(ndp):
            wfull[k * rows:(k + 1) * rows, :feat] = wall[k].astype(F32)
        wt[:, :width] = jnp.transpose(wfull[...])[:feat].astype(BF16)

        def project(part, c):
            lhs = wt[c * ROWS:(c + 1) * ROWS, part * TILE:(part + 1) * TILE]
            for q in mxus:
                pltpu.matmul_acc_lhs(proj[q][c], lhs, load_staged_rhs=part if c == 0 else None)

        def push_gradient(k, g):
            for q in mxus:
                pltpu.matmul_push_rhs(x_tile(PAIR * k + g, q), staging_register=g, mxu_index=q)

        def gradient(s_ref, g):
            lhs = s_ref[:, g * patches:(g + 1) * patches]
            for q in mxus:
                pltpu.matmul_acc_lhs(grad_acc[q], lhs, load_staged_rhs=g)

        def keep(p_ref, c):
            for q in mxus:
                p_ref[q, c * ROWS:(c + 1) * ROWS, :] = pltpu.matmul_pop(proj[q][c])

        def pointwise(p_ref, s_ref, k, c, stat, loss):
            for f in range(c * ROWS, (c + 1) * ROWS, CHUNK):
                total = jnp.zeros((CHUNK, LANES), F32)
                for g in range(PAIR):
                    for h in range(halves):
                        lanes = slice(h * LANES, (h + 1) * LANES)
                        r, m, cov = [v[:, lanes] for v in stat[g]]
                        t = tv[PAIR * k + g, h, f:f + CHUNK, :].astype(F32)
                        differ = p_ref[g, f:f + CHUNK, lanes] + (m - t * r)
                        clipped = jnp.clip(differ, -1.0, 1.0)
                        source = clipped * cov
                        loss[h] = loss[h] + source * (differ - 0.5 * clipped)
                        total = total + source
                        if f < early:
                            s2[PAIR * k + g, h, f:f + CHUNK, :] = source.astype(BF16)
                        else:
                            at = g * patches + h * LANES
                            s_ref[f - early:f - early + CHUNK, at:at + LANES] = source.astype(BF16)
                gacc[f:f + CHUNK, :] += total

        def step(k, p_in, p_out, s_out, s_in):
            last = steps - 1
            back, ahead, beyond = jnp.maximum(k - 1, 0), jnp.minimum(k + 1, last), jnp.minimum(k + 2, last)
            stat = [[v[pl.ds(PAIR * k + g, 1), :] for v in (rbuf, mbuf, cbuf)] for g in range(PAIR)]
            loss = [jnp.zeros((CHUNK, LANES), F32)] * halves
            todo = [functools.partial(project, 0, c) for c in range(pieces)]
            todo.append(functools.partial(push_project, ahead, 1))
            todo += [functools.partial(project, 1, c) for c in range(pieces)]
            todo.append(functools.partial(push_gradient, back, 0))
            todo.append(functools.partial(gradient, s_in, 0))
            todo.append(functools.partial(push_gradient, back, 1))
            todo.append(functools.partial(push_project, beyond, 0))
            todo.append(functools.partial(gradient, s_in, 1))
            done = 0
            for c in range(pieces):
                upto = min(len(todo), pl.cdiv(len(todo) * (c + 1), pieces))
                for op in todo[done:upto]:
                    op()
                done = upto
                pointwise(p_in, s_out, k, c, stat, loss)
            for c in range(pieces):
                keep(p_out, c)
            lacc[...] += functools.reduce(jnp.add, loss)

        for part in range(2):
            for c in range(pieces):
                project(part, c)
        push_project(1, 0)
        for c in range(pieces):
            keep(pa, c)
        per_group = GROUP // PAIR

        def outer(g, _):
            @pl.when(g + 1 < groups)
            def _():
                x_wait(g + 1)

            arrive(srecv.at[:, g], srs.at[g])
            parts_in = [ssend[g]] + [srecv[o - 1, g] for o in range(1, nmp)]
            sums = [p[:GROUP] for p in parts_in]
            mean = functools.reduce(jnp.add, sums) * (1.0 / feat_full)
            var = functools.reduce(jnp.add, [p[GROUP:] for p in parts_in])
            for s in sums:
                gap = s * (1.0 / feat) - mean
                var = var + feat * (gap * gap)
            rstd = lax.rsqrt(var * (1.0 / feat_full) + 1e-05)
            here = pl.ds(pl.multiple_of(g * GROUP, GROUP), GROUP)
            rbuf[here, :] = rstd
            mbuf[here, :] = mean * rstd

            def inner(j, _):
                k = g * per_group + 2 * j
                step(k, pa, pb, sa, sb)
                pl.delay(1)
                step(k + 1, pb, pa, sb, sa)
                return 0

            lax.fori_loop(0, per_group // 2, inner, 0)
            return 0

        lax.fori_loop(0, groups, outer, 0)
        project(0, 0)
        for q in mxus:
            pltpu.matmul_pop(proj[q][0])
        for g in range(PAIR):
            push_gradient(steps - 1, g)
            gradient(sb, g)
        acc1[:rest, :TILE] = pltpu.matmul_pop(grad_acc[0])
        acc1[:rest, TILE:] = pltpu.matmul_pop(grad_acc[1])[:, :width - TILE]

        half_at, sums_at, late_at, total_rows = layout(rows)
        tiles = featp // LANES
        bias_part = jnp.sum(jnp.transpose(gacc[...]), axis=0, keepdims=True)
        loss_part = jnp.sum(lacc[...], keepdims=True)
        count_part = jnp.sum(cbuf[...], keepdims=True)
        at_row = lax.broadcasted_iota(jnp.int32, (8, LANES), 0)
        extra = jnp.where(at_row == tiles, loss_part, count_part)
        for n in range(tiles):
            extra = jnp.where(at_row == n, bias_part[:, n * LANES:(n + 1) * LANES], extra)
        full = jnp.transpose(acc1[...])
        half = LANES // 2
        for k in range(ndp):
            slot = gs1.at[k % inner_dp, k // inner_dp]
            mine = full[k * rows:(k + 1) * rows]
            slot[:rows, :] = mine[:, :LANES]
            hs[k // inner_dp, k % inner_dp, :rows // 2, :] = jnp.concatenate(
                [mine[:rows // 2, LANES:LANES + half], mine[rows // 2:, LANES:LANES + half]], axis=1)
            slot[half_at:, :] = extra

        def p_copy(o, bufs):
            src, dst, _, _, ss, rs, _, _ = bufs
            to = lax.rem(far + o, outer_dp)
            return pltpu.make_async_remote_copy(
                src_ref=src.at[other, to], dst_ref=dst.at[o], send_sem=ss, recv_sem=rs.at[o],
                device_id=(partner, mp), device_id_type=MESH)

        def g_copy(o, bufs):
            _, _, src, dst, _, _, ss, rs = bufs
            return pltpu.make_async_remote_copy(
                src_ref=src.at[o - 1], dst_ref=dst.at[o - 1], send_sem=ss, recv_sem=rs,
                device_id=(line(o), mp), device_id_type=MESH)

        first = (gs1, pv1, gm1, gr1, ps1, pr1, g1s, g1r)
        second = (gs2, pv2, gm2, gr2, ps2, pr2, g2s, g2r)
        order = [ranked(1, n) for n in reversed(range(outer_dp - 1))] + [0]

        def h_copy(o):
            to = lax.rem(far + o, outer_dp)
            return pltpu.make_async_remote_copy(
                src_ref=hs.at[to], dst_ref=hr.at[o - 1], send_sem=hss, recv_sem=hrs,
                device_id=(line(o), mp), device_id_type=MESH)

        h_pair = pltpu.make_async_remote_copy(
            src_ref=ht.at[other], dst_ref=hv, send_sem=hps, recv_sem=hpr,
            device_id=(partner, mp), device_id_type=MESH)
        for o in order[:-1]:
            h_copy(o).start()
        for o in order:
            p_copy(o, first).start()

        def push_late(img, r):
            for q in mxus:
                pltpu.matmul_push_rhs(x_tile(img, q), staging_register=r, mxu_index=q)

        push_late(0, 0)

        def sweep(k, _):
            for g in range(SWEEP):
                img = k * SWEEP + g
                push_late(jnp.minimum(img + 1, images - 1), (g + 1) % 2)
                lhs = jnp.concatenate([s2[img, h, :, :] for h in range(halves)], axis=1)
                for q in mxus:
                    pltpu.matmul_acc_lhs(late_acc[q], lhs, load_staged_rhs=g % 2)
            return 0

        lax.fori_loop(0, images // SWEEP, sweep, 0)
        acc2[:, :TILE] = pltpu.matmul_pop(late_acc[0])
        acc2[:, TILE:] = pltpu.matmul_pop(late_acc[1])[:, :width - TILE]
        for q in mxus:
            pltpu.matmul_acc_lhs(late_acc[q], jnp.zeros((early, TILE), BF16), load_staged_rhs=0)
            pltpu.matmul_pop(late_acc[q])
        full = jnp.transpose(acc2[...])
        for k in range(ndp):
            gs2[k % inner_dp, k // inner_dp, :rows, :] = full[k * rows:(k + 1) * rows]
        for o in order:
            p_copy(o, second).start()

        pairs = []
        for bufs in (first, second):
            src, dst, mid_buf = bufs[:3]
            for o in order:
                p_copy(o, bufs).wait_recv()
                pair = src[near, lax.rem(far + o, outer_dp)] + dst[o]
                if o is not order[-1]:
                    mid_buf[o - 1] = pair
                    g_copy(o, bufs).start()
            pairs.append(pair)
            if bufs is first:
                arrive(hr, hrs)
                both = hs[far]
                for o in range(outer_dp - 1):
                    both = both + hr[o]
                ht[...] = both
                h_pair.start()
        for n, bufs in enumerate((first, second)):
            arrive(bufs[3], bufs[7])
            for o in range(1, outer_dp):
                pairs[n] = pairs[n] + bufs[3][o - 1]
        h_pair.wait_recv()
        packed = ht[near] + hv[...]
        outv[:half_at, :] = pairs[0][:half_at]
        outv[half_at:sums_at, :] = packed
        outv[sums_at:late_at, :] = pairs[0][half_at:]
        outv[late_at:total_rows, :] = pairs[1]
        head = pairs[0][:half_at]
        sums = pairs[0][half_at:]
        bias_grad = sums[:tiles]
        square = jnp.sum(head * head, keepdims=True) + jnp.sum(pairs[1] * pairs[1], keepdims=True)
        square = square + jnp.sum(packed * packed, keepdims=True)
        bias_square = jnp.sum(bias_grad * bias_grad, keepdims=True)
        lane = lax.broadcasted_iota(jnp.int32, (1, LANES), 1)
        fsend[...] = jnp.where(lane == 0, square + bias_square * (1.0 / ndp), sums[tiles:tiles + 1, :])

        def f_copy(d):
            return pltpu.make_async_remote_copy(
                src_ref=fsend, dst_ref=frecv.at[me], send_sem=fss, recv_sem=frs,
                device_id=(d // nmp, lax.rem(d, nmp)), device_id_type=MESH)

        def f_start(o, _):
            f_copy(o + jnp.where(o >= me, 1, 0)).start()
            return 0

        lax.fori_loop(0, ntot - 1, f_start, 0)
        frecv[me] = fsend[...]
        arrive(wall.at[pl.ds(0, outer_dp - 1)], wss)
        arrive(wall.at[pl.ds(0, outer_dp)], whs)
        arrive(hs.at[pl.ds(0, outer_dp - 1)], hss)
        h_pair.wait_send()
        for bufs in (first, second):
            arrive(bufs[0].at[0], bufs[4])
            arrive(bufs[2], bufs[6])
        arrive(srecv, sss)
        everyone = frecv.at[pl.ds(0, ntot - 1)]
        arrive(everyone, frs)
        outv[total_rows:, :] = jnp.broadcast_to(jnp.sum(frecv[...], axis=0), (8, LANES))
        arrive(everyone, fss)

    tile = [pltpu.ACC(q)((ROWS, TILE), F32) for q in mxus]
    refs = [tile[0]] * pieces + [tile[1]] * pieces
    refs += [pltpu.ACC(q)((rest, TILE), F32) for q in mxus]
    refs += [pltpu.ACC(q)((early, TILE), F32) for q in mxus]
    pl.run_scoped(scoped, *refs)


def body(pred_input, proj_weight, proj_bias, targets, block_masks):
    images, patches, width = pred_input.shape
    feat = targets.shape[2]
    rows = proj_weight.shape[0]
    blocks = block_masks.shape[1]
    ndp, nmp = lax.axis_size("dp"), lax.axis_size("mp")
    ntot = ndp * nmp
    featp = pad_to(feat, LANES)
    groups = images // GROUP
    halves, parts = patches // LANES, width // LANES
    early = LANES
    rest = feat - early
    dma = pltpu.SemaphoreType.DMA
    vmem = pl.BlockSpec(memory_space=pltpu.VMEM)
    hbm = pl.BlockSpec(memory_space=pl.ANY)
    half_at, sums_at, late_at, total_rows = layout(rows)
    inner_dp = 2
    outer_dp = ndp // inner_dp
    exchange = []
    for n in (half_at + 8, total_rows - late_at):
        exchange += [
            pltpu.VMEM((inner_dp, outer_dp, n, LANES), F32),
            pltpu.VMEM((outer_dp, n, LANES), F32),
            pltpu.VMEM((outer_dp - 1, n, LANES), F32),
            pltpu.VMEM((outer_dp - 1, n, LANES), F32),
        ]
    held = sums_at - half_at
    exchange += [
        pltpu.VMEM((outer_dp, inner_dp, held, LANES), F32),
        pltpu.VMEM((outer_dp - 1, inner_dp, held, LANES), F32),
        pltpu.VMEM((inner_dp, held, LANES), F32),
        pltpu.VMEM((held, LANES), F32),
    ]
    exchange_sems = [dma(()), dma((outer_dp,)), dma(()), dma(())]
    summed = pl.pallas_call(
        functools.partial(kernel, ndp, nmp),
        out_shape=pltpu.VMEM((total_rows + 8, LANES), F32),
        in_specs=[hbm] * 5,
        out_specs=vmem,
        scratch_shapes=[
            pltpu.VMEM((parts, images * patches, LANES), BF16),
            pltpu.VMEM((images, halves, feat, LANES), BF16),
            pltpu.VMEM((images, blocks, patches), jnp.int32),
            pltpu.VMEM((rows, feat), BF16),
            pltpu.VMEM((feat,), F32),
            pltpu.VMEM((ndp, rows, feat), BF16),
            pltpu.VMEM((width, featp), F32),
            pltpu.VMEM((feat, pad_to(width, TILE)), BF16),
            pltpu.VMEM((patches, LANES), BF16),
            pltpu.VMEM((featp, LANES), F32),
            pltpu.VMEM((8, featp), F32),
            pltpu.VMEM((groups, 2 * GROUP, patches), F32),
            pltpu.VMEM((nmp - 1, groups, 2 * GROUP, patches), F32),
            pltpu.VMEM((images, patches), F32),
            pltpu.VMEM((images, patches), F32),
            pltpu.VMEM((images, patches), F32),
            pltpu.VMEM((PAIR, feat, patches), F32),
            pltpu.VMEM((PAIR, feat, patches), F32),
            pltpu.VMEM((rest, PAIR * patches), BF16),
            pltpu.VMEM((rest, PAIR * patches), BF16),
            pltpu.VMEM((images, halves, early, LANES), BF16),
            pltpu.VMEM((pad_to(rest, LANES), width), F32),
            pltpu.VMEM((early, width), F32),
            pltpu.VMEM((featp, LANES), F32),
            pltpu.VMEM((CHUNK, LANES), F32),
        ] + exchange + [
            pltpu.VMEM((1, LANES), F32),
            pltpu.VMEM((ntot, 1, LANES), F32),
            dma((groups,)), dma((groups,)), dma((2,)), dma(()),
            dma(()), dma((outer_dp,)), dma(()), dma(()), dma(()), dma((groups,)),
        ] + exchange_sems * 2 + [dma(())] * 6,
        compiler_params=pltpu.CompilerParams(
            collective_id=0, has_side_effects=True, vmem_limit_bytes=60 * 1024 * 1024
        ),
    )(
        pred_input.reshape(images * patches, width),
        proj_weight,
        proj_bias,
        jnp.swapaxes(targets, 1, 2),
        block_masks,
    )
    loss, clip, gw, gb = pl.pallas_call(
        functools.partial(finish, ndp, nmp),
        out_shape=(
            jax.ShapeDtypeStruct((1, 1), F32),
            jax.ShapeDtypeStruct((1, 1), F32),
            jax.ShapeDtypeStruct((rows, feat), F32),
            jax.ShapeDtypeStruct((feat,), F32),
        ),
        in_specs=[vmem],
        out_specs=(vmem,) * 4,
    )(pltpu.with_memory_space_constraint(summed, pltpu.VMEM))
    return loss.reshape(()), clip.reshape(()), gw, gb


def solution(mesh):
    in_specs = (
        P("dp", None, None),
        P("dp", "mp"),
        P("mp"),
        P("dp", None, "mp"),
        P("dp", None, None),
    )
    out_specs = (P(), P(), P("dp", "mp"), P("mp"))
    return jax.shard_map(body, mesh=mesh, in_specs=in_specs, out_specs=out_specs, check_vma=False)
```

```python
import functools

import jax
import jax.numpy as jnp
from jax import lax
from jax.experimental import pallas as pl
from jax.experimental.pallas import tpu as pltpu
from jax.sharding import PartitionSpec as P

F32 = jnp.float32
BF16 = jnp.bfloat16
MESH = pl.DeviceIdType.MESH
LANES = 128
GROUP = 8
PAIR = 2
CHUNK = 16
TILE = 256
ROWS = 16
SWEEP = 32
HANDS = (6, 7)


def pad_to(n, m):
    return (n + m - 1) // m * m


def layout(rows):
    half = pad_to(rows, 8)
    sums = half + pad_to(rows // 2, 8)
    late = sums + 8
    return half, sums, late, late + pad_to(rows, 8)


def finish(ndp, nmp, sum_ref, loss_ref, clip_ref, gw_ref, gb_ref):
    rows, feat = gw_ref.shape
    half_at, sums_at, late_at, fin_at = layout(rows)
    tiles = pad_to(feat, LANES) // LANES
    count = sum_ref[sums_at + tiles + 1:sums_at + tiles + 2, 0:1]
    square, loss = sum_ref[fin_at:fin_at + 1, 0:1], sum_ref[fin_at:fin_at + 1, 1:2]
    norm = jnp.sqrt(square) / count
    scale = jnp.minimum(1.0, 1.0 / (norm + 1e-06))
    factor = scale / count
    loss_ref[...] = loss / count * (1.0 / (feat * nmp * ndp))
    clip_ref[...] = scale
    gw_ref[:, :LANES] = sum_ref[late_at:late_at + rows, :] * factor
    gw_ref[:, LANES:2 * LANES] = sum_ref[:rows, :] * factor
    half = LANES // 2
    packed = sum_ref[half_at:half_at + rows // 2, :] * factor
    gw_ref[:rows // 2, 2 * LANES:] = packed[:, :half]
    gw_ref[rows // 2:, 2 * LANES:] = packed[:, half:]
    for n in range(tiles):
        stop = min((n + 1) * LANES, feat)
        bias = sum_ref[sums_at + n:sums_at + n + 1, :] * factor
        gb_ref[n * LANES:stop] = bias[0, :stop - n * LANES]


def kernel(ndp, nmp, x_hbm, w_hbm, b_hbm, t_hbm, m_hbm,
           outv,
           xv, tv, mv, w_ref, b_ref, wall, wfull, wt, ones, bcol, brow, ssend, srecv, rbuf, mbuf, cbuf,
           pa, pb, sa, sb, s2, acc1, acc2, gacc, lacc,
           gs1, pv1, gm1, gr1, gs2, pv2, gm2, gr2, hs, hr, ht, hv, fsend, frecv,
           xsem, tsem, msem, bsem, wss, wrs, whs, whr, sss, srs, ps1, pr1, g1s, g1r, ps2, pr2, g2s, g2r, hss, hrs, hps, hpr, fss, frs):
    images, halves, feat, _ = tv.shape
    patches = halves * LANES
    parts, _, _ = xv.shape
    width = parts * LANES
    rows = w_ref.shape[0]
    early = s2.shape[2]
    rest = feat - early
    pieces = feat // ROWS
    dp, mp = lax.axis_index("dp"), lax.axis_index("mp")
    inner_dp, outer_dp = gs1.shape[0], gs1.shape[1]
    near, far = lax.rem(dp, inner_dp), dp // inner_dp
    featp = bcol.shape[0]
    groups = images // GROUP
    steps = images // PAIR
    ntot = ndp * nmp
    me = dp * nmp + mp
    feat_full = feat * nmp
    mxus = range(2)

    def scoped(*accs):
        proj = [list(accs[q * pieces:(q + 1) * pieces]) for q in mxus]
        grad_acc = list(accs[2 * pieces:2 * pieces + 2])
        late_acc = list(accs[2 * pieces + 2:2 * pieces + 4])

        def t_copy(g, h):
            s = pl.ds(g * GROUP, GROUP)
            return pltpu.make_async_copy(t_hbm.at[s, :, pl.ds(h * LANES, LANES)], tv.at[s, h], tsem.at[g])

        def x_copy(g, j):
            s = pl.ds(g * GROUP * patches, GROUP * patches)
            return pltpu.make_async_copy(x_hbm.at[s, pl.ds(j * LANES, LANES)], xv.at[j, s], xsem.at[g])

        def x_start(g):
            for j in range(parts):
                x_copy(g, j).start()

        def arrive(ref, sem):
            pltpu.make_async_copy(ref, ref, sem).wait()

        def x_wait(g):
            arrive(xv.at[:, pl.ds(g * GROUP * patches, GROUP * patches)], xsem.at[g])

        m_copy = pltpu.make_async_copy(m_hbm, mv, msem.at[0])
        w_own = pltpu.make_async_copy(w_hbm, w_ref, msem.at[1])
        b_own = pltpu.make_async_copy(b_hbm, b_ref, bsem)
        barrier = pltpu.get_barrier_semaphore()

        other = 1 - near

        def line(o):
            return lax.rem(far + o, outer_dp) * inner_dp + near

        partner = far * inner_dp + other
        peers = [(line(o), mp) for o in range(1, outer_dp)] + [(partner, mp)]
        peers += [(dp, lax.rem(mp + o, nmp)) for o in range(1, nmp)]
        for peer in peers:
            pl.semaphore_signal(barrier, inc=1, device_id=peer, device_id_type=MESH)
        w_own.start()
        b_own.start()
        m_copy.start()
        for g in range(groups):
            for h in range(halves):
                t_copy(g, h).start()

        pl.semaphore_wait(barrier, len(peers))

        def w_copy(o):
            return pltpu.make_async_remote_copy(
                src_ref=w_ref, dst_ref=wall.at[dp], send_sem=wss, recv_sem=wrs.at[o],
                device_id=(line(o), mp), device_id_type=MESH)

        def w_hand(o):
            src = lax.rem(far - o + outer_dp, outer_dp) * inner_dp + near
            own = isinstance(o, int) and o == 0
            return pltpu.make_async_remote_copy(
                src_ref=w_ref if own else wall.at[src], dst_ref=wall.at[src], send_sem=whs, recv_sem=whr,
                device_id=(partner, mp), device_id_type=MESH)

        def ranked(offset, n):
            picks = 0
            for f in range(outer_dp):
                near_first = sorted(range(1, outer_dp), key=lambda o: abs((f + offset * o) % outer_dp - f))
                picks = picks + jnp.where(far == f, near_first[n], 0)
            return picks

        w_own.wait()
        for n in reversed(range(outer_dp - 1)):
            w_copy(ranked(1, n)).start()
        w_hand(0).start()

        def x_tile(img, part):
            at = pl.ds(pl.multiple_of(img * patches, patches), patches)
            left = xv[2 * part, at, :]
            right = xv[2 * part + 1, at, :] if 2 * part + 1 < parts else ones[...]
            return jnp.concatenate([left, right], axis=1)

        def push_project(k, part):
            for q in mxus:
                tile = x_tile(PAIR * k + q, part)
                pltpu.matmul_push_rhs(tile, staging_register=part, mxu_index=q, transpose=True)

        def s_copy(o, g):
            return pltpu.make_async_remote_copy(
                src_ref=ssend.at[g], dst_ref=srecv.at[o - 1, g],
                send_sem=sss, recv_sem=srs.at[g],
                device_id=(dp, lax.rem(mp + o, nmp)), device_id_type=MESH)

        def stats(g, _):
            arrive(tv.at[pl.ds(g * GROUP, GROUP)], tsem.at[g])

            @pl.when(g >= 2)
            def _():
                x_start(g - 2)

            sums, squares = [], []
            for j in range(GROUP):
                i = g * GROUP + j
                for h in range(halves):
                    part = jnp.zeros((CHUNK, LANES), F32)
                    for c in range(0, feat, CHUNK):
                        part = part + tv[i, h, c:c + CHUNK, :].astype(F32)
                    total = jnp.sum(part, axis=0, keepdims=True)
                    mean = total * (1.0 / feat)
                    part = jnp.zeros((CHUNK, LANES), F32)
                    for c in range(0, feat, CHUNK):
                        centred = tv[i, h, c:c + CHUNK, :].astype(F32) - mean
                        part = part + centred * centred
                    sums.append(total)
                    squares.append(jnp.sum(part, axis=0, keepdims=True))
            for h in range(halves):
                block = jnp.concatenate(sums[h::halves] + squares[h::halves], axis=0)
                ssend[g, :, h * LANES:(h + 1) * LANES] = block

            @pl.when(g > 0)
            def _():
                for o in range(1, nmp):
                    s_copy(o, g - 1).start()

            for n in range(min(outer_dp - 1, len(HANDS))):
                pl.when(g == HANDS[n])(functools.partial(hand_over, n))

            return 0

        def hand_over(n):
            src = n + jnp.where(n >= far, 1, 0)
            o = lax.rem(far - src + outer_dp, outer_dp)
            w_copy(o).wait_recv()
            w_hand(o).start()

        lax.fori_loop(0, groups, stats, 0)
        for g in range(groups - 2, groups):
            x_start(g)

        for o in range(1, nmp):
            s_copy(o, groups - 1).start()
        for n in range(len(HANDS), outer_dp - 1):
            hand_over(n)
        gacc[...] = jnp.zeros_like(gacc)
        lacc[...] = jnp.zeros_like(lacc)
        sb[...] = jnp.zeros_like(sb)
        acc1[...] = jnp.zeros_like(acc1)
        wfull[...] = jnp.zeros_like(wfull)
        brow[...] = jnp.zeros_like(brow)
        if rows % 16:
            gs1[...] = jnp.zeros_like(gs1)
            gs2[...] = jnp.zeros_like(gs2)
            hs[...] = jnp.zeros_like(hs)
        lane = lax.broadcasted_iota(jnp.int32, ones.shape, 1)
        ones[...] = jnp.where(lane < 3, 1.0, 0.0).astype(BF16)
        b_own.wait()
        brow[0:1, :feat] = b_ref[...].reshape(1, feat)
        bcol[...] = jnp.transpose(jnp.broadcast_to(brow[0:1, :], (LANES, featp)))
        bias = bcol[:feat, :]
        high = bias.astype(BF16)
        left = bias - high.astype(F32)
        mid = left.astype(BF16)
        low = (left - mid.astype(F32)).astype(BF16)
        lane = lax.broadcasted_iota(jnp.int32, (feat, LANES), 1)
        pick = jnp.where(lane == 0, high.astype(F32), jnp.where(lane == 1, mid.astype(F32), low.astype(F32)))
        wt[:, width:] = jnp.where(lane < 3, pick, 0.0).astype(BF16)
        for q in mxus:
            blank = jnp.zeros((ROWS, TILE), BF16)
            pltpu.matmul_acc_lhs(proj[q][0], blank, load_staged_rhs=0)
            pltpu.matmul_acc_lhs(proj[q][0], blank, load_staged_rhs=1)
            for ref in proj[q] + [grad_acc[q], late_acc[q]]:
                pltpu.matmul_pop(ref)

        m_copy.wait()

        def cover(g, _):
            block = [jnp.sum(mv[g * GROUP + j], axis=0, keepdims=True) for j in range(GROUP)]
            cbuf[pl.ds(pl.multiple_of(g * GROUP, GROUP), GROUP), :] = jnp.concatenate(block, axis=0).astype(F32)
            return 0

        lax.fori_loop(0, groups, cover, 0)

        x_wait(0)
        for part in range(2):
            push_project(0, part)
        wall[dp] = w_ref[...]
        arrive(wall.at[pl.ds(0, outer_dp)], whr)
        for k in range(ndp):
            wfull[k * rows:(k + 1) * rows, :feat] = wall[k].astype(F32)
        wt[:, :width] = jnp.transpose(wfull[...])[:feat].astype(BF16)

        def project(part, c):
            lhs = wt[c * ROWS:(c + 1) * ROWS, part * TILE:(part + 1) * TILE]
            for q in mxus:
                pltpu.matmul_acc_lhs(proj[q][c], lhs, load_staged_rhs=part if c == 0 else None)

        def push_gradient(k, g):
            for q in mxus:
                pltpu.matmul_push_rhs(x_tile(PAIR * k + g, q), staging_register=g, mxu_index=q)

        def gradient(s_ref, g):
            lhs = s_ref[:, g * patches:(g + 1) * patches]
            for q in mxus:
                pltpu.matmul_acc_lhs(grad_acc[q], lhs, load_staged_rhs=g)

        def keep(p_ref, c):
            for q in mxus:
                p_ref[q, c * ROWS:(c + 1) * ROWS, :] = pltpu.matmul_pop(proj[q][c])

        def pointwise(p_ref, s_ref, k, c, stat, loss):
            for f in range(c * ROWS, (c + 1) * ROWS, CHUNK):
                total = jnp.zeros((CHUNK, LANES), F32)
                for g in range(PAIR):
                    for h in range(halves):
                        lanes = slice(h * LANES, (h + 1) * LANES)
                        r, m, cov = [v[:, lanes] for v in stat[g]]
                        t = tv[PAIR * k + g, h, f:f + CHUNK, :].astype(F32)
                        differ = p_ref[g, f:f + CHUNK, lanes] + (m - t * r)
                        clipped = jnp.clip(differ, -1.0, 1.0)
                        source = clipped * cov
                        loss[h] = loss[h] + source * (differ - 0.5 * clipped)
                        total = total + source
                        if f < early:
                            s2[PAIR * k + g, h, f:f + CHUNK, :] = source.astype(BF16)
                        else:
                            at = g * patches + h * LANES
                            s_ref[f - early:f - early + CHUNK, at:at + LANES] = source.astype(BF16)
                gacc[f:f + CHUNK, :] += total

        def step(k, p_in, p_out, s_out, s_in):
            last = steps - 1
            back, ahead, beyond = jnp.maximum(k - 1, 0), jnp.minimum(k + 1, last), jnp.minimum(k + 2, last)
            stat = [[v[pl.ds(PAIR * k + g, 1), :] for v in (rbuf, mbuf, cbuf)] for g in range(PAIR)]
            loss = [jnp.zeros((CHUNK, LANES), F32)] * halves
            todo = [functools.partial(project, 0, c) for c in range(pieces)]
            todo.append(functools.partial(push_project, ahead, 1))
            todo += [functools.partial(project, 1, c) for c in range(pieces)]
            todo.append(functools.partial(push_gradient, back, 0))
            todo.append(functools.partial(gradient, s_in, 0))
            todo.append(functools.partial(push_gradient, back, 1))
            todo.append(functools.partial(push_project, beyond, 0))
            todo.append(functools.partial(gradient, s_in, 1))
            done = 0
            for c in range(pieces):
                upto = min(len(todo), pl.cdiv(len(todo) * (c + 1), pieces))
                for op in todo[done:upto]:
                    op()
                done = upto
                pointwise(p_in, s_out, k, c, stat, loss)
            for c in range(pieces):
                keep(p_out, c)
            lacc[...] += functools.reduce(jnp.add, loss)

        for part in range(2):
            for c in range(pieces):
                project(part, c)
        push_project(1, 0)
        for c in range(pieces):
            keep(pa, c)
        per_group = GROUP // PAIR

        def outer(g, _):
            @pl.when(g + 1 < groups)
            def _():
                x_wait(g + 1)

            arrive(srecv.at[:, g], srs.at[g])
            parts_in = [ssend[g]] + [srecv[o - 1, g] for o in range(1, nmp)]
            sums = [p[:GROUP] for p in parts_in]
            mean = functools.reduce(jnp.add, sums) * (1.0 / feat_full)
            var = functools.reduce(jnp.add, [p[GROUP:] for p in parts_in])
            for s in sums:
                gap = s * (1.0 / feat) - mean
                var = var + feat * (gap * gap)
            rstd = lax.rsqrt(var * (1.0 / feat_full) + 1e-05)
            here = pl.ds(pl.multiple_of(g * GROUP, GROUP), GROUP)
            rbuf[here, :] = rstd
            mbuf[here, :] = mean * rstd

            def inner(j, _):
                k = g * per_group + 2 * j
                step(k, pa, pb, sa, sb)
                pl.delay(1)
                step(k + 1, pb, pa, sb, sa)
                return 0

            lax.fori_loop(0, per_group // 2, inner, 0)
            return 0

        lax.fori_loop(0, groups, outer, 0)
        project(0, 0)
        for g in range(PAIR):
            push_gradient(steps - 1, g)
            gradient(sb, g)
        acc1[:rest, :TILE] = pltpu.matmul_pop(grad_acc[0])
        acc1[:rest, TILE:] = pltpu.matmul_pop(grad_acc[1])[:, :width - TILE]
        for q in mxus:
            pltpu.matmul_pop(proj[q][0])

        half_at, sums_at, late_at, total_rows = layout(rows)
        tiles = featp // LANES
        bias_part = jnp.sum(jnp.transpose(gacc[...]), axis=0, keepdims=True)
        loss_part = jnp.sum(lacc[...], keepdims=True)
        count_part = jnp.sum(cbuf[...], keepdims=True)
        at_row = lax.broadcasted_iota(jnp.int32, (8, LANES), 0)
        extra = jnp.where(at_row == tiles, loss_part, count_part)
        for n in range(tiles):
            extra = jnp.where(at_row == n, bias_part[:, n * LANES:(n + 1) * LANES], extra)
        full = jnp.transpose(acc1[...])
        half = LANES // 2
        for k in range(ndp):
            slot = gs1.at[k % inner_dp, k // inner_dp]
            mine = full[k * rows:(k + 1) * rows]
            slot[:rows, :] = mine[:, :LANES]
            hs[k // inner_dp, k % inner_dp, :rows // 2, :] = jnp.concatenate(
                [mine[:rows // 2, LANES:LANES + half], mine[rows // 2:, LANES:LANES + half]], axis=1)
            slot[half_at:, :] = extra

        def p_copy(o, bufs):
            src, dst, _, _, ss, rs, _, _ = bufs
            to = lax.rem(far + o, outer_dp)
            return pltpu.make_async_remote_copy(
                src_ref=src.at[other, to], dst_ref=dst.at[o], send_sem=ss, recv_sem=rs.at[o],
                device_id=(partner, mp), device_id_type=MESH)

        def g_copy(o, bufs):
            _, _, src, dst, _, _, ss, rs = bufs
            return pltpu.make_async_remote_copy(
                src_ref=src.at[o - 1], dst_ref=dst.at[o - 1], send_sem=ss, recv_sem=rs,
                device_id=(line(o), mp), device_id_type=MESH)

        first = (gs1, pv1, gm1, gr1, ps1, pr1, g1s, g1r)
        second = (gs2, pv2, gm2, gr2, ps2, pr2, g2s, g2r)
        order = [ranked(1, n) for n in reversed(range(outer_dp - 1))] + [0]

        def h_copy(o):
            to = lax.rem(far + o, outer_dp)
            return pltpu.make_async_remote_copy(
                src_ref=hs.at[to], dst_ref=hr.at[o - 1], send_sem=hss, recv_sem=hrs,
                device_id=(line(o), mp), device_id_type=MESH)

        h_pair = pltpu.make_async_remote_copy(
            src_ref=ht.at[other], dst_ref=hv, send_sem=hps, recv_sem=hpr,
            device_id=(partner, mp), device_id_type=MESH)
        for o in order[:-1]:
            h_copy(o).start()
        for o in order:
            p_copy(o, first).start()

        def push_late(img, r):
            for q in mxus:
                pltpu.matmul_push_rhs(x_tile(img, q), staging_register=r, mxu_index=q)

        push_late(0, 0)

        def sweep(k, _):
            for g in range(SWEEP):
                img = k * SWEEP + g
                push_late(jnp.minimum(img + 1, images - 1), (g + 1) % 2)
                lhs = jnp.concatenate([s2[img, h, :, :] for h in range(halves)], axis=1)
                for q in mxus:
                    pltpu.matmul_acc_lhs(late_acc[q], lhs, load_staged_rhs=g % 2)
            return 0

        lax.fori_loop(0, images // SWEEP, sweep, 0)
        acc2[:, :TILE] = pltpu.matmul_pop(late_acc[0])
        acc2[:, TILE:] = pltpu.matmul_pop(late_acc[1])[:, :width - TILE]
        full = jnp.transpose(acc2[...])
        for k in range(ndp):
            gs2[k % inner_dp, k // inner_dp, :rows, :] = full[k * rows:(k + 1) * rows]
        for o in order:
            p_copy(o, second).start()
        for q in mxus:
            pltpu.matmul_acc_lhs(late_acc[q], jnp.zeros((early, TILE), BF16), load_staged_rhs=0)
            pltpu.matmul_pop(late_acc[q])

        pairs = []
        for bufs in (first, second):
            src, dst, mid_buf = bufs[:3]
            for o in order:
                p_copy(o, bufs).wait_recv()
                pair = src[near, lax.rem(far + o, outer_dp)] + dst[o]
                if o is not order[-1]:
                    mid_buf[o - 1] = pair
                    g_copy(o, bufs).start()
            pairs.append(pair)
            if bufs is first:
                arrive(hr, hrs)
                both = hs[far]
                for o in range(outer_dp - 1):
                    both = both + hr[o]
                ht[...] = both
                h_pair.start()
        for n, bufs in enumerate((first, second)):
            arrive(bufs[3], bufs[7])
            for o in range(1, outer_dp):
                pairs[n] = pairs[n] + bufs[3][o - 1]
        h_pair.wait_recv()
        packed = ht[near] + hv[...]
        outv[:half_at, :] = pairs[0][:half_at]
        outv[half_at:sums_at, :] = packed
        outv[sums_at:late_at, :] = pairs[0][half_at:]
        outv[late_at:total_rows, :] = pairs[1]
        head = pairs[0][:half_at]
        sums = pairs[0][half_at:]
        bias_grad = sums[:tiles]
        square = jnp.sum(head * head, keepdims=True) + jnp.sum(pairs[1] * pairs[1], keepdims=True)
        square = square + jnp.sum(packed * packed, keepdims=True)
        bias_square = jnp.sum(bias_grad * bias_grad, keepdims=True)
        lane = lax.broadcasted_iota(jnp.int32, (1, LANES), 1)
        fsend[...] = jnp.where(lane == 0, square + bias_square * (1.0 / ndp), sums[tiles:tiles + 1, :])

        def f_copy(d):
            return pltpu.make_async_remote_copy(
                src_ref=fsend, dst_ref=frecv.at[me], send_sem=fss, recv_sem=frs,
                device_id=(d // nmp, lax.rem(d, nmp)), device_id_type=MESH)

        def f_start(o, _):
            f_copy(o + jnp.where(o >= me, 1, 0)).start()
            return 0

        lax.fori_loop(0, ntot - 1, f_start, 0)
        frecv[me] = fsend[...]
        arrive(wall.at[pl.ds(0, outer_dp - 1)], wss)
        arrive(wall.at[pl.ds(0, outer_dp)], whs)
        arrive(hs.at[pl.ds(0, outer_dp - 1)], hss)
        h_pair.wait_send()
        for bufs in (first, second):
            arrive(bufs[0].at[0], bufs[4])
            arrive(bufs[2], bufs[6])
        arrive(srecv, sss)
        everyone = frecv.at[pl.ds(0, ntot - 1)]
        arrive(everyone, frs)
        outv[total_rows:, :] = jnp.broadcast_to(jnp.sum(frecv[...], axis=0), (8, LANES))
        arrive(everyone, fss)

    tile = [pltpu.ACC(q)((ROWS, TILE), F32) for q in mxus]
    refs = [tile[0]] * pieces + [tile[1]] * pieces
    refs += [pltpu.ACC(q)((rest, TILE), F32) for q in mxus]
    refs += [pltpu.ACC(q)((early, TILE), F32) for q in mxus]
    pl.run_scoped(scoped, *refs)


def body(pred_input, proj_weight, proj_bias, targets, block_masks):
    images, patches, width = pred_input.shape
    feat = targets.shape[2]
    rows = proj_weight.shape[0]
    blocks = block_masks.shape[1]
    ndp, nmp = lax.axis_size("dp"), lax.axis_size("mp")
    ntot = ndp * nmp
    featp = pad_to(feat, LANES)
    groups = images // GROUP
    halves, parts = patches // LANES, width // LANES
    early = LANES
    rest = feat - early
    dma = pltpu.SemaphoreType.DMA
    vmem = pl.BlockSpec(memory_space=pltpu.VMEM)
    hbm = pl.BlockSpec(memory_space=pl.ANY)
    half_at, sums_at, late_at, total_rows = layout(rows)
    inner_dp = 2
    outer_dp = ndp // inner_dp
    exchange = []
    for n in (half_at + 8, total_rows - late_at):
        exchange += [
            pltpu.VMEM((inner_dp, outer_dp, n, LANES), F32),
            pltpu.VMEM((outer_dp, n, LANES), F32),
            pltpu.VMEM((outer_dp - 1, n, LANES), F32),
            pltpu.VMEM((outer_dp - 1, n, LANES), F32),
        ]
    held = sums_at - half_at
    exchange += [
        pltpu.VMEM((outer_dp, inner_dp, held, LANES), F32),
        pltpu.VMEM((outer_dp - 1, inner_dp, held, LANES), F32),
        pltpu.VMEM((inner_dp, held, LANES), F32),
        pltpu.VMEM((held, LANES), F32),
    ]
    exchange_sems = [dma(()), dma((outer_dp,)), dma(()), dma(())]
    summed = pl.pallas_call(
        functools.partial(kernel, ndp, nmp),
        out_shape=pltpu.VMEM((total_rows + 8, LANES), F32),
        in_specs=[hbm] * 5,
        out_specs=vmem,
        scratch_shapes=[
            pltpu.VMEM((parts, images * patches, LANES), BF16),
            pltpu.VMEM((images, halves, feat, LANES), BF16),
            pltpu.VMEM((images, blocks, patches), jnp.int32),
            pltpu.VMEM((rows, feat), BF16),
            pltpu.VMEM((feat,), F32),
            pltpu.VMEM((ndp, rows, feat), BF16),
            pltpu.VMEM((width, featp), F32),
            pltpu.VMEM((feat, pad_to(width, TILE)), BF16),
            pltpu.VMEM((patches, LANES), BF16),
            pltpu.VMEM((featp, LANES), F32),
            pltpu.VMEM((8, featp), F32),
            pltpu.VMEM((groups, 2 * GROUP, patches), F32),
            pltpu.VMEM((nmp - 1, groups, 2 * GROUP, patches), F32),
            pltpu.VMEM((images, patches), F32),
            pltpu.VMEM((images, patches), F32),
            pltpu.VMEM((images, patches), F32),
            pltpu.VMEM((PAIR, feat, patches), F32),
            pltpu.VMEM((PAIR, feat, patches), F32),
            pltpu.VMEM((rest, PAIR * patches), BF16),
            pltpu.VMEM((rest, PAIR * patches), BF16),
            pltpu.VMEM((images, halves, early, LANES), BF16),
            pltpu.VMEM((pad_to(rest, LANES), width), F32),
            pltpu.VMEM((early, width), F32),
            pltpu.VMEM((featp, LANES), F32),
            pltpu.VMEM((CHUNK, LANES), F32),
        ] + exchange + [
            pltpu.VMEM((1, LANES), F32),
            pltpu.VMEM((ntot, 1, LANES), F32),
            dma((groups,)), dma((groups,)), dma((2,)), dma(()),
            dma(()), dma((outer_dp,)), dma(()), dma(()), dma(()), dma((groups,)),
        ] + exchange_sems * 2 + [dma(())] * 6,
        compiler_params=pltpu.CompilerParams(
            collective_id=0, has_side_effects=True, vmem_limit_bytes=60 * 1024 * 1024
        ),
    )(
        pred_input.reshape(images * patches, width),
        proj_weight,
        proj_bias,
        jnp.swapaxes(targets, 1, 2),
        block_masks,
    )
    loss, clip, gw, gb = pl.pallas_call(
        functools.partial(finish, ndp, nmp),
        out_shape=(
            jax.ShapeDtypeStruct((1, 1), F32),
            jax.ShapeDtypeStruct((1, 1), F32),
            jax.ShapeDtypeStruct((rows, feat), F32),
            jax.ShapeDtypeStruct((feat,), F32),
        ),
        in_specs=[vmem],
        out_specs=(vmem,) * 4,
    )(pltpu.with_memory_space_constraint(summed, pltpu.VMEM))
    return loss.reshape(()), clip.reshape(()), gw, gb


def solution(mesh):
    in_specs = (
        P("dp", None, None),
        P("dp", "mp"),
        P("mp"),
        P("dp", None, "mp"),
        P("dp", None, None),
    )
    out_specs = (P(), P(), P("dp", "mp"), P("mp"))
    return jax.shard_map(body, mesh=mesh, in_specs=in_specs, out_specs=out_specs, check_vma=False)
```
